32 devices in a mesh: dp: 2 (over x), tp: 4 (over z), cp: 4 (over y, core).
Axes of the slice: x: 2, y: 2, z: 4, core: 2. Of those that a mesh axis runs over, the one named last changes fastest.
Arguments:
- hidden_in: bfloat16 [4096, 3584], P(('dp', 'cp', 'tp')), parts along dimension 0
- positions: int32 [4096], P(('dp', 'cp', 'tp')), parts along dimension 0
- cache_len: int32 [2], P('dp'), parts along dimension 0
- cache_k: bfloat16 [8192, 512], P(('dp', 'cp', 'tp')), parts along dimension 0
- cache_v: bfloat16 [8192, 512], P(('dp', 'cp', 'tp')), parts along dimension 0
- norm1_gain: bfloat16 [3584], replicated
- w_query: bfloat16 [3584, 3584], P(None, 'tp')
- w_key: bfloat16 [3584, 512], P(None, 'tp')
- w_value: bfloat16 [3584, 512], P(None, 'tp')
- w_out: bfloat16 [3584, 3584], P('tp')
- norm2_gain: bfloat16 [3584], replicated
- w_gate: bfloat16 [3584, 18944], P(None, 'tp')
- w_up: bfloat16 [3584, 18944], P(None, 'tp')
- w_down: bfloat16 [18944, 3584], P('tp')
Outputs:
- output: bfloat16 [4096, 3584], P(('dp', 'cp', 'tp')), parts along dimension 0
There are 2 independent parts. The reference program is written for one: setup_inputs(seed, part) draws one part's arguments, and reference() takes and returns one part's arrays. A program takes and returns all parts, laid end to end along the dimension named above; an argument that names none is the same for every part.
All inputs are finite; a program needn't handle non-finite values.
Results may differ from the reference program's by a relative error of at most 0.0108171.
Values are sent between devices in bfloat16 or wider.
A program may use at most 1 GiB of HBM per device.

```python
import math
import jax
import jax.numpy as jnp
from jax import lax

TOKENS = 2048
PREFIX = 4096
D_MODEL = 3584
Q_HEADS = 28
KV_HEADS = 4
HEAD_DIM = 128
FFN_DIM = 18944
SHARD_COUNT = 16
SHARD_ROWS = 128
QUERY_BLOCK = 64
ROPE_BASE = 500000.0
NORM_EPS = 1e-5


def normal_draw(rand_key, out_shape, spread):
    return (jax.random.normal(rand_key, out_shape, jnp.float32) * spread).astype(jnp.bfloat16)


def setup_inputs(seed: int = 0, part: int = 0) -> dict:
    base_key = jax.random.key(seed)
    part_keys = jax.random.split(jax.random.fold_in(base_key, part), 4)
    shared_keys = jax.random.split(jax.random.key(seed + 1), 9)
    cache_len = jax.random.randint(part_keys[0], (1,), PREFIX // 16, PREFIX + 1, dtype=jnp.int32)
    row_ids = jnp.arange(TOKENS, dtype=jnp.int32)
    half_rows = SHARD_ROWS // 2
    shard_ids = row_ids // SHARD_ROWS
    within = row_ids % SHARD_ROWS
    segment = jnp.where(within < half_rows, shard_ids, 2 * SHARD_COUNT - 1 - shard_ids)
    positions = cache_len[0] + segment * half_rows + within % half_rows
    qk_std = math.log((PREFIX + TOKENS) / 4.0) ** 0.25
    width_std = D_MODEL ** -0.5
    kv_width = KV_HEADS * HEAD_DIM
    return {
        'hidden_in': normal_draw(part_keys[1], (TOKENS, D_MODEL), 1.0),
        'positions': positions,
        'cache_len': cache_len,
        'cache_k': normal_draw(part_keys[2], (PREFIX, kv_width), qk_std),
        'cache_v': normal_draw(part_keys[3], (PREFIX, kv_width), 1.0),
        'norm1_gain': (1.0 + 0.3 * jax.random.normal(shared_keys[0], (D_MODEL,), jnp.float32)).astype(jnp.bfloat16),
        'w_query': normal_draw(shared_keys[1], (D_MODEL, Q_HEADS * HEAD_DIM), qk_std * width_std),
        'w_key': normal_draw(shared_keys[2], (D_MODEL, kv_width), qk_std * width_std),
        'w_value': normal_draw(shared_keys[3], (D_MODEL, kv_width), width_std),
        'w_out': normal_draw(shared_keys[4], (Q_HEADS * HEAD_DIM, D_MODEL), 2.0 * (Q_HEADS * HEAD_DIM) ** -0.5),
        'norm2_gain': (1.0 + 0.3 * jax.random.normal(shared_keys[5], (D_MODEL,), jnp.float32)).astype(jnp.bfloat16),
        'w_gate': normal_draw(shared_keys[6], (D_MODEL, FFN_DIM), width_std),
        'w_up': normal_draw(shared_keys[7], (D_MODEL, FFN_DIM), width_std),
        'w_down': normal_draw(shared_keys[8], (FFN_DIM, D_MODEL), FFN_DIM ** -0.5),
    }


def rms_norm(hidden, norm_gain):
    values = hidden.astype(jnp.float32)
    inv_rms = lax.rsqrt(jnp.mean(values * values, axis=-1, keepdims=True) + NORM_EPS)
    return (values * inv_rms * norm_gain.astype(jnp.float32)).astype(jnp.bfloat16)


def rotary(projected, positions):
    half_dim = HEAD_DIM // 2
    inv_freq = 1.0 / (ROPE_BASE ** (jnp.arange(half_dim, dtype=jnp.float32) * (2.0 / HEAD_DIM)))
    angles = positions.astype(jnp.float32)[:, None] * inv_freq[None, :]
    expand = (angles.shape[0],) + (1,) * (projected.ndim - 2) + (half_dim,)
    cos_table = jnp.cos(angles).reshape(expand)
    sin_table = jnp.sin(angles).reshape(expand)
    first_half = projected[..., :half_dim]
    second_half = projected[..., half_dim:]
    rotated = jnp.concatenate([first_half * cos_table - second_half * sin_table, second_half * cos_table + first_half * sin_table], axis=-1)
    return rotated.astype(jnp.bfloat16)


def reference(hidden_in, positions, cache_len, cache_k, cache_v, norm1_gain, w_query, w_key, w_value, w_out, norm2_gain, w_gate, w_up, w_down):
    groups = Q_HEADS // KV_HEADS
    block_count = TOKENS // QUERY_BLOCK
    score_scale = 1.0 / math.sqrt(HEAD_DIM)
    normed = rms_norm(hidden_in, norm1_gain)
    queries = rotary(jnp.dot(normed, w_query, preferred_element_type=jnp.float32).reshape(TOKENS, KV_HEADS, groups, HEAD_DIM), positions)
    new_keys = rotary(jnp.dot(normed, w_key, preferred_element_type=jnp.float32).reshape(TOKENS, KV_HEADS, HEAD_DIM), positions)
    new_values = jnp.dot(normed, w_value, preferred_element_type=jnp.float32).astype(jnp.bfloat16).reshape(TOKENS, KV_HEADS, HEAD_DIM)
    head_keys = jnp.moveaxis(new_keys, 1, 0)
    head_values = jnp.moveaxis(new_values, 1, 0)
    cached_keys = jnp.moveaxis(cache_k.reshape(PREFIX, KV_HEADS, HEAD_DIM), 1, 0)
    cached_values = jnp.moveaxis(cache_v.reshape(PREFIX, KV_HEADS, HEAD_DIM), 1, 0)
    cache_valid = jnp.arange(PREFIX) < cache_len[0]
    query_blocks = jnp.moveaxis(queries.reshape(block_count, QUERY_BLOCK, KV_HEADS, groups, HEAD_DIM), 2, 1)
    position_blocks = positions.reshape(block_count, QUERY_BLOCK)

    def attend_block(block_item):
        block_queries, block_pos = block_item
        causal = positions[None, None, :] <= block_pos[None, :, None]

        def attend_head(head_item):
            head_queries, cache_key_head, cache_value_head, new_key_head, new_value_head = head_item
            query_wide = head_queries.astype(jnp.float32)
            cache_scores = jnp.einsum('rgd,sd->grs', query_wide, cache_key_head.astype(jnp.float32)) * score_scale
            new_scores = jnp.einsum('rgd,sd->grs', query_wide, new_key_head.astype(jnp.float32)) * score_scale
            cache_scores = jnp.where(cache_valid[None, None, :], cache_scores, -jnp.inf)
            new_scores = jnp.where(causal, new_scores, -jnp.inf)
            row_max = jnp.maximum(jnp.max(cache_scores, axis=-1, keepdims=True), jnp.max(new_scores, axis=-1, keepdims=True))
            cache_probs = jnp.exp(cache_scores - row_max)
            new_probs = jnp.exp(new_scores - row_max)
            normalizer = jnp.sum(cache_probs, axis=-1, keepdims=True) + jnp.sum(new_probs, axis=-1, keepdims=True)
            weighted = jnp.einsum('grs,sd->grd', cache_probs.astype(jnp.bfloat16).astype(jnp.float32), cache_value_head.astype(jnp.float32))
            weighted = weighted + jnp.einsum('grs,sd->grd', new_probs.astype(jnp.bfloat16).astype(jnp.float32), new_value_head.astype(jnp.float32))
            return (weighted / normalizer).astype(jnp.bfloat16)

        return lax.map(attend_head, (block_queries, cached_keys, cached_values, head_keys, head_values))

    attended = lax.map(attend_block, (query_blocks, position_blocks))
    attended = jnp.transpose(attended, (0, 3, 1, 2, 4)).reshape(TOKENS, Q_HEADS * HEAD_DIM)
    residual_mid = (hidden_in.astype(jnp.float32) + jnp.dot(attended, w_out, preferred_element_type=jnp.float32)).astype(jnp.bfloat16)
    normed_mid = rms_norm(residual_mid, norm2_gain)
    gate_proj = jnp.dot(normed_mid, w_gate, preferred_element_type=jnp.float32)
    up_proj = jnp.dot(normed_mid, w_up, preferred_element_type=jnp.float32)
    hidden_mlp = (jax.nn.silu(gate_proj) * up_proj).astype(jnp.bfloat16)
    return (residual_mid.astype(jnp.float32) + jnp.dot(hidden_mlp, w_down, preferred_element_type=jnp.float32)).astype(jnp.bfloat16)
```

```python
import functools
import math
import jax
import jax.numpy as jnp
from jax import lax
from jax.experimental import pallas as pl
from jax.experimental.pallas import tpu as pltpu
from jax.sharding import PartitionSpec as P

HEAD_DIM = 128
ROPE_BASE = 500000.0
NORM_EPS = 1e-5
RUN = 64
KV_BLOCK = 512
LOG2E = 1.4426950408889634


def rms_norm(hidden, norm_gain):
    values = hidden.astype(jnp.float32)
    inv_rms = lax.rsqrt(jnp.mean(values * values, axis=-1, keepdims=True) + NORM_EPS)
    return (values * inv_rms * norm_gain.astype(jnp.float32)).astype(jnp.bfloat16)


def rotary(projected, cos_table, sin_table):
    half_dim = HEAD_DIM // 2
    cos_table = cos_table[:, None, :]
    sin_table = sin_table[:, None, :]
    first_half = projected[..., :half_dim]
    second_half = projected[..., half_dim:]
    rotated = jnp.concatenate([first_half * cos_table - second_half * sin_table, second_half * cos_table + first_half * sin_table], axis=-1)
    return rotated.astype(jnp.bfloat16)


def attn_kernel(clen_ref, q_ref, kc_ref, vc_ref, knl_ref, vnl_ref, knh_ref, vnh_ref, o_ref, m_ref, l_ref, acc_ref):
    cp = lax.axis_index('cp')
    scale = LOG2E / math.sqrt(HEAD_DIM)
    half = q_ref.shape[0] // 2
    cache_len = clen_ref[0]
    m_ref[...] = jnp.full_like(m_ref, -1e30)
    l_ref[...] = jnp.zeros_like(l_ref)
    acc_ref[...] = jnp.zeros_like(acc_ref)

    def update(row0, rows, keys, values, mask=None):
        span = pl.ds(row0, rows)
        queries = q_ref[span, :]
        scores = lax.dot_general(queries, keys, (((1,), (1,)), ((), ())), preferred_element_type=jnp.float32) * scale
        if mask is not None:
            scores = jnp.where(mask, scores, -jnp.inf)
        width = scores.shape[1]
        m_old = m_ref[span, :]
        m_new = jnp.maximum(m_old, jnp.max(scores, axis=1, keepdims=True))
        probs = jnp.exp2(scores - m_new[:, :1])
        alpha = jnp.exp2(m_old - m_new)
        part = probs[:, :HEAD_DIM]
        for j in range(1, width // HEAD_DIM):
            part = part + probs[:, j * HEAD_DIM:(j + 1) * HEAD_DIM]
        l_ref[span, :] = alpha * l_ref[span, :] + part
        acc_ref[span, :] = alpha * acc_ref[span, :] + jnp.dot(probs.astype(jnp.bfloat16), values, preferred_element_type=jnp.float32)
        m_ref[span, :] = m_new

    full_blocks = cache_len // KV_BLOCK

    def cache_step(j, carry):
        rows = pl.ds(pl.multiple_of(j * KV_BLOCK, KV_BLOCK), KV_BLOCK)
        update(0, 2 * half, kc_ref[rows, :], vc_ref[rows, :])
        return carry

    lax.fori_loop(0, full_blocks, cache_step, 0)

    @pl.when(full_blocks * KV_BLOCK < cache_len)
    def _():
        rows = pl.ds(pl.multiple_of(full_blocks * KV_BLOCK, KV_BLOCK), KV_BLOCK)
        slots = full_blocks * KV_BLOCK + lax.broadcasted_iota(jnp.int32, (2 * half, KV_BLOCK), 1)
        update(0, 2 * half, kc_ref[rows, :], vc_ref[rows, :], slots < cache_len)

    def low_keys(j):
        rows = pl.ds(pl.multiple_of(j * half, half), half)
        return knl_ref[rows, :], vnl_ref[rows, :]

    def high_keys(j):
        rows = pl.ds(pl.multiple_of(j * half, half), half)
        return knh_ref[rows, :], vnh_ref[rows, :]

    def both_step(j, carry):
        update(0, 2 * half, *low_keys(j))
        return carry

    lax.fori_loop(0, cp, both_step, 0)
    row_id = lax.broadcasted_iota(jnp.int32, (half, half), 0)
    col_id = lax.broadcasted_iota(jnp.int32, (half, half), 1)
    update(0, half, *low_keys(cp), col_id <= row_id)
    update(half, half, *low_keys(cp))

    def high_low_step(j, carry):
        update(half, half, *low_keys(j))
        return carry

    lax.fori_loop(cp + 1, 4, high_low_step, 0)

    def high_high_step(j, carry):
        update(half, half, *high_keys(j))
        return carry

    lax.fori_loop(cp + 1, 4, high_high_step, 0)
    runs = half // RUN

    def place(i):
        return (runs - 1 - i // RUN) * RUN + i % RUN

    update(half, half, *high_keys(cp), place(col_id) <= place(row_id))
    total = jnp.sum(l_ref[...], axis=1, keepdims=True)
    o_ref[...] = (acc_ref[...] / total).astype(jnp.bfloat16)


def attention(cache_len, queries, cache_keys, cache_values, low_keys, low_values, high_keys, high_values):
    rows, width = queries.shape
    heads = width // HEAD_DIM

    def whole(array):
        return pl.BlockSpec(array.shape, lambda g: (0, 0))

    return pl.pallas_call(
        attn_kernel,
        grid=(heads,),
        out_shape=jax.ShapeDtypeStruct((rows, width), jnp.bfloat16),
        in_specs=[pl.BlockSpec(memory_space=pltpu.SMEM), pl.BlockSpec((rows, HEAD_DIM), lambda g: (0, g))]
        + [whole(a) for a in (cache_keys, cache_values, low_keys, low_values, high_keys, high_values)],
        out_specs=pl.BlockSpec((rows, HEAD_DIM), lambda g: (0, g)),
        scratch_shapes=[pltpu.VMEM((rows, HEAD_DIM), jnp.float32)] * 3,
        cost_estimate=pl.CostEstimate(flops=2 * 2 * rows * width * 4608, bytes_accessed=8 * 2**20, transcendentals=rows * heads * 4608),
        name='attend',
    )(cache_len, queries, cache_keys, cache_values, low_keys, low_values, high_keys, high_values)


def solution(mesh):
    tp_size, cp_size, dp_size = mesh.shape['tp'], mesh.shape['cp'], mesh.shape['dp']
    token_spec = P(('dp', 'cp', 'tp'), None)
    column_spec = P(None, 'tp')
    row_spec = P('tp', None)

    def device_layer(hidden_loc, pos_loc, cache_len, cache_k, cache_v, norm1_gain, w_query, w_key, w_value, w_out, norm2_gain, w_gate, w_up, w_down):
        shard_rows, d_model = hidden_loc.shape
        heads_width = w_query.shape[1]
        dp, tp, cp = lax.axis_index('dp'), lax.axis_index('tp'), lax.axis_index('cp')
        normed = rms_norm(hidden_loc, norm1_gain)
        inv_freq = 1.0 / (ROPE_BASE ** (jnp.arange(HEAD_DIM // 2, dtype=jnp.float32) * (2.0 / HEAD_DIM)))

        def swap_cache(cache):
            swapped = lax.all_to_all(cache, 'tp', 1, 0, tiled=True)
            return lax.all_gather(swapped, 'cp', axis=0, tiled=True)

        cache_keys, cache_values = swap_cache(cache_k), swap_cache(cache_v)

        def project(index):
            rows_in = lax.all_gather(normed[index * RUN:(index + 1) * RUN], 'tp', axis=0, tiled=True)
            runs = cp * tp_size + jnp.arange(tp_size)
            if index == 1:
                runs = 2 * cp_size * tp_size - 1 - runs
            positions = cache_len[0] + (runs[:, None] * RUN + jnp.arange(RUN)[None, :]).reshape(-1)
            angles = positions.astype(jnp.float32)[:, None] * inv_freq[None, :]
            cos_table, sin_table = jnp.cos(angles), jnp.sin(angles)

            def rotated(weight):
                wide = jnp.dot(rows_in, weight, preferred_element_type=jnp.float32).reshape(rows_in.shape[0], -1, HEAD_DIM)
                return rotary(wide, cos_table, sin_table).reshape(rows_in.shape[0], -1)

            keys = rotated(w_key)
            values = jnp.dot(rows_in, w_value, preferred_element_type=jnp.float32).astype(jnp.bfloat16)
            queries = rotated(w_query)
            keys, values = (lax.all_gather(a, 'cp', axis=0, tiled=True) for a in (keys, values))
            return rows_in, queries, keys, values

        rows_low, q_low, k_low, v_low = project(0)
        rows_high, q_high, k_high, v_high = project(1)

        piece_rows = w_out.shape[0] // (dp_size * cp_size)
        piece = lax.dynamic_slice_in_dim(w_out, (dp * cp_size + cp) * piece_rows, piece_rows, 0)
        piece, rows_high = lax.optimization_barrier((piece, rows_high))
        w_out_all = lax.all_gather(piece, ('dp', 'tp', 'cp'), axis=0, tiled=True)

        attended = attention(cache_len, jnp.concatenate([q_low, q_high], axis=0), cache_keys, cache_values, k_low, v_low, k_high, v_high)
        attended = jnp.transpose(attended.reshape(2, tp_size, RUN, heads_width), (1, 0, 2, 3))
        attended = lax.all_to_all(attended, 'tp', 0, 0, tiled=True).reshape(tp_size, shard_rows, dp_size, heads_width // dp_size)
        attended = jnp.transpose(attended, (1, 2, 0, 3)).reshape(shard_rows, -1)
        attn_out = jnp.dot(attended, w_out_all, preferred_element_type=jnp.float32)
        residual_mid = (hidden_loc.astype(jnp.float32) + attn_out).astype(jnp.bfloat16)
        normed_mid = rms_norm(residual_mid, norm2_gain)

        outs = []
        for index in range(2):
            rows = slice(index * RUN, (index + 1) * RUN)
            group_mid = lax.all_gather(normed_mid[rows], 'tp', axis=0, tiled=True)
            gate_proj = jnp.dot(group_mid, w_gate, preferred_element_type=jnp.float32)
            up_proj = jnp.dot(group_mid, w_up, preferred_element_type=jnp.float32)
            hidden_mlp = (jax.nn.silu(gate_proj) * up_proj).astype(jnp.bfloat16)
            mlp_part = jnp.dot(hidden_mlp, w_down, preferred_element_type=jnp.float32)
            summed = lax.psum_scatter(mlp_part, 'tp', scatter_dimension=0, tiled=True)
            outs.append((residual_mid[rows].astype(jnp.float32) + summed).astype(jnp.bfloat16))
        return jnp.concatenate(outs, axis=0)

    return jax.shard_map(device_layer, mesh=mesh, in_specs=(token_spec, P(('dp', 'cp', 'tp')), P('dp'), token_spec, token_spec, P(), column_spec, column_spec, column_spec, row_spec, P(), column_spec, column_spec, row_spec), out_specs=token_spec, check_vma=False)
```

```python
import functools
import math
import jax
import jax.numpy as jnp
from jax import lax
from jax.experimental import pallas as pl
from jax.experimental.pallas import tpu as pltpu
from jax.sharding import PartitionSpec as P

HEAD_DIM = 128
ROPE_BASE = 500000.0
NORM_EPS = 1e-5
RUN = 64
KV_BLOCK = 512
LOG2E = 1.4426950408889634


def rms_norm(hidden, norm_gain):
    values = hidden.astype(jnp.float32)
    inv_rms = lax.rsqrt(jnp.mean(values * values, axis=-1, keepdims=True) + NORM_EPS)
    return (values * inv_rms * norm_gain.astype(jnp.float32)).astype(jnp.bfloat16)


def rotary(projected, cos_table, sin_table):
    half_dim = HEAD_DIM // 2
    cos_table = cos_table[:, None, :]
    sin_table = sin_table[:, None, :]
    first_half = projected[..., :half_dim]
    second_half = projected[..., half_dim:]
    rotated = jnp.concatenate([first_half * cos_table - second_half * sin_table, second_half * cos_table + first_half * sin_table], axis=-1)
    return rotated.astype(jnp.bfloat16)


def attn_kernel(clen_ref, q_ref, kc_ref, vc_ref, knl_ref, vnl_ref, knh_ref, vnh_ref, o_ref, vt_ref, m_ref, l_ref, acc_ref):
    cp = lax.axis_index('cp')
    scale = LOG2E / math.sqrt(HEAD_DIM)
    half = q_ref.shape[0] // 2
    slots = kc_ref.shape[0]
    fresh = knl_ref.shape[0]
    cache_len = clen_ref[0]

    @pl.when(pl.program_id(0) == 0)
    def _():
        for ref, base in ((vc_ref, 0), (vnl_ref, slots), (vnh_ref, slots + fresh)):
            for j in range(ref.shape[0] // 512):
                block = ref[j * 512:(j + 1) * 512, :].astype(jnp.float32)
                vt_ref[:, base + j * 512:base + (j + 1) * 512] = block.T.astype(jnp.bfloat16)

    m_ref[...] = jnp.full_like(m_ref, -1e30)
    l_ref[...] = jnp.zeros_like(l_ref)
    acc_ref[...] = jnp.zeros_like(acc_ref)

    def update(parts, keys, vt_cols, masks=(None, None)):
        scores = {}
        for part in parts:
            raw = lax.dot_general(keys, q_ref[part * half:(part + 1) * half, :], (((1,), (1,)), ((), ())), preferred_element_type=jnp.float32)
            scores[part] = raw if masks[part] is None else jnp.where(masks[part], raw, -jnp.inf)
        for part in parts:
            cols = slice(part * half, (part + 1) * half)
            m_old = m_ref[:, cols]
            m_new = jnp.maximum(m_old, jnp.max(scores[part], axis=0, keepdims=True))
            probs = jnp.exp2((scores[part] - m_new) * scale)
            alpha = jnp.exp2((m_old - m_new) * scale)
            l_ref[:, cols] = alpha * l_ref[:, cols] + jnp.sum(probs, axis=0, keepdims=True)
            acc_ref[:, cols] = alpha * acc_ref[:, cols] + jnp.dot(vt_ref[:, vt_cols], probs.astype(jnp.bfloat16), preferred_element_type=jnp.float32)
            m_ref[:, cols] = m_new

    full_blocks = cache_len // KV_BLOCK

    def cache_step(j, carry):
        rows = pl.ds(pl.multiple_of(j * KV_BLOCK, KV_BLOCK), KV_BLOCK)
        update((0, 1), kc_ref[rows, :], rows)
        return carry

    lax.fori_loop(0, full_blocks, cache_step, 0)

    @pl.when(full_blocks * KV_BLOCK < cache_len)
    def _():
        rows = pl.ds(pl.multiple_of(full_blocks * KV_BLOCK, KV_BLOCK), KV_BLOCK)
        visible = full_blocks * KV_BLOCK + lax.broadcasted_iota(jnp.int32, (KV_BLOCK, half), 0) < cache_len
        update((0, 1), kc_ref[rows, :], rows, (visible, visible))

    def new_keys(ref, base, j):
        start = pl.multiple_of(j * half, half)
        return ref[pl.ds(start, half), :], pl.ds(pl.multiple_of(base + start, half), half)

    def both_step(j, carry):
        update((0, 1), *new_keys(knl_ref, slots, j))
        return carry

    lax.fori_loop(0, cp, both_step, 0)
    key_id = lax.broadcasted_iota(jnp.int32, (half, half), 0)
    row_id = lax.broadcasted_iota(jnp.int32, (half, half), 1)
    update((0, 1), *new_keys(knl_ref, slots, cp), (key_id <= row_id, None))

    def high_step(j, carry):
        update((1,), *new_keys(knl_ref, slots, j))
        update((1,), *new_keys(knh_ref, slots + fresh, j))
        return carry

    lax.fori_loop(cp + 1, 4, high_step, 0)
    runs = half // RUN

    def place(i):
        return (runs - 1 - i // RUN) * RUN + i % RUN

    update((1,), *new_keys(knh_ref, slots + fresh, cp), (None, place(key_id) <= place(row_id)))
    o_ref[...] = (acc_ref[...] / l_ref[...]).T.astype(jnp.bfloat16)


def attention(cache_len, queries, cache_kv, low_kv, high_kv, head0, heads):
    rows = queries.shape[0]

    def column(array, index):
        return pl.BlockSpec((array.shape[0], HEAD_DIM), lambda g: (0, index))

    arrays = (cache_kv, low_kv, high_kv)
    return pl.pallas_call(
        attn_kernel,
        grid=(heads,),
        out_shape=jax.ShapeDtypeStruct((rows, heads * HEAD_DIM), jnp.bfloat16),
        in_specs=[pl.BlockSpec(memory_space=pltpu.SMEM), pl.BlockSpec((rows, HEAD_DIM), lambda g: (0, g + head0))]
        + [column(a, i) for a in arrays for i in range(2)],
        out_specs=pl.BlockSpec((rows, HEAD_DIM), lambda g: (0, g)),
        scratch_shapes=[pltpu.VMEM((HEAD_DIM, sum(a.shape[0] for a in arrays)), jnp.bfloat16)] + [pltpu.VMEM((1, rows), jnp.float32)] * 2 + [pltpu.VMEM((HEAD_DIM, rows), jnp.float32)],
        cost_estimate=pl.CostEstimate(flops=2 * 2 * rows * heads * HEAD_DIM * 4608, bytes_accessed=8 * 2**20, transcendentals=rows * heads * 4608),
        name='attend',
    )(cache_len, queries, *[a for a in arrays for _ in range(2)])


def solution(mesh):
    tp_size, cp_size, dp_size = mesh.shape['tp'], mesh.shape['cp'], mesh.shape['dp']
    token_spec = P(('dp', 'cp', 'tp'), None)
    column_spec = P(None, 'tp')
    row_spec = P('tp', None)

    def device_layer(hidden_loc, pos_loc, cache_len, cache_k, cache_v, norm1_gain, w_query, w_key, w_value, w_out, norm2_gain, w_gate, w_up, w_down):
        shard_rows, d_model = hidden_loc.shape
        heads_width = w_query.shape[1]
        dp, tp, cp = lax.axis_index('dp'), lax.axis_index('tp'), lax.axis_index('cp')
        normed = rms_norm(hidden_loc, norm1_gain)
        inv_freq = 1.0 / (ROPE_BASE ** (jnp.arange(HEAD_DIM // 2, dtype=jnp.float32) * (2.0 / HEAD_DIM)))

        def place(parts, me):
            size = len(parts)
            out = jnp.zeros((size,) + parts[0].shape, parts[0].dtype)
            for shift, part in enumerate(parts):
                out = lax.dynamic_update_index_in_dim(out, part, (me - shift) % size, 0)
            return out

        def shifted(part, axis_name, size, shift):
            return part if shift == 0 else lax.ppermute(part, axis_name, [(i, (i + shift) % size) for i in range(size)])

        def share(block):
            return place([shifted(block, 'cp', cp_size, shift) for shift in range(cp_size)], cp).reshape(-1, block.shape[-1])

        def exchange(block, split_axis):
            pieces = [lax.dynamic_index_in_dim(block, (tp + shift) % tp_size, split_axis, keepdims=False) for shift in range(tp_size)]
            return place([shifted(piece, 'tp', tp_size, shift) for shift, piece in enumerate(pieces)], tp)

        slots = cache_k.shape[0]
        cache_kv = jnp.stack([cache_k.reshape(slots, tp_size, HEAD_DIM), cache_v.reshape(slots, tp_size, HEAD_DIM)], axis=2)
        cache_kv = jnp.transpose(cache_kv.reshape(slots, tp_size, 2 * HEAD_DIM), (1, 0, 2))
        cache_kv = share(exchange(cache_kv, 0).reshape(tp_size * slots, 2 * HEAD_DIM))

        def project(index):
            rows_in = lax.all_gather(normed[index * RUN:(index + 1) * RUN], 'tp', axis=0, tiled=True)
            runs = cp * tp_size + jnp.arange(tp_size)
            if index == 1:
                runs = 2 * cp_size * tp_size - 1 - runs
            positions = cache_len[0] + (runs[:, None] * RUN + jnp.arange(RUN)[None, :]).reshape(-1)
            angles = positions.astype(jnp.float32)[:, None] * inv_freq[None, :]
            cos_table, sin_table = jnp.cos(angles), jnp.sin(angles)

            def rotated(weight):
                wide = jnp.dot(rows_in, weight, preferred_element_type=jnp.float32).reshape(rows_in.shape[0], -1, HEAD_DIM)
                return rotary(wide, cos_table, sin_table).reshape(rows_in.shape[0], -1)

            values = jnp.dot(rows_in, w_value, preferred_element_type=jnp.float32).astype(jnp.bfloat16)
            shared = share(jnp.concatenate([rotated(w_key), values], axis=1))
            return rows_in, rotated(w_query), shared

        rows_low, q_low, low_kv = project(0)
        rows_high, q_high, high_kv = project(1)

        core, row_y = cp % 2, cp // 2
        piece_rows = w_out.shape[0] // (dp_size * cp_size)
        half_rows = w_out.shape[0] // 2
        piece = lax.dynamic_slice_in_dim(w_out, core * half_rows + (dp * 2 + row_y) * piece_rows, piece_rows, 0)
        piece, cache_kv, low_kv, q_low, rows_high = lax.optimization_barrier((piece, cache_kv, low_kv, q_low, rows_high))
        groups = [[(d * tp_size + t) * cp_size + 2 * y + k for d in range(dp_size) for t in range(tp_size) for y in range(cp_size // 2)] for k in range(2)]
        w_out_mine = lax.all_gather(piece, ('dp', 'tp', 'cp'), axis_index_groups=groups, axis=0, tiled=True)

        queries = jnp.concatenate([q_low, q_high], axis=0)
        groups_of_heads = []
        for head0, heads in ((0, 4), (4, 3)):
            attended = attention(cache_len, queries, cache_kv, low_kv, high_kv, head0, heads)
            attended = exchange(attended.reshape(2, tp_size, RUN, heads * HEAD_DIM), 1)
            groups_of_heads.append(attended.reshape(tp_size, shard_rows, heads * HEAD_DIM))
        attended = jnp.concatenate(groups_of_heads, axis=2).reshape(tp_size, shard_rows, 2, dp_size, -1)
        attended = jnp.transpose(attended, (2, 1, 3, 0, 4)).reshape(2, shard_rows, -1)
        attended, w_out_mine = lax.optimization_barrier((attended, w_out_mine))
        w_out_other = lax.ppermute(w_out_mine, 'cp', [(i, i ^ 1) for i in range(cp_size)])
        attn_out = jnp.dot(lax.dynamic_index_in_dim(attended, core, 0, keepdims=False), w_out_mine, preferred_element_type=jnp.float32)
        attn_out = attn_out + jnp.dot(lax.dynamic_index_in_dim(attended, 1 - core, 0, keepdims=False), w_out_other, preferred_element_type=jnp.float32)
        residual_mid = (hidden_loc.astype(jnp.float32) + attn_out).astype(jnp.bfloat16)
        normed_mid = rms_norm(residual_mid, norm2_gain)

        outs = []
        for index in range(2):
            rows = slice(index * RUN, (index + 1) * RUN)
            group_mid = lax.all_gather(normed_mid[rows], 'tp', axis=0, tiled=True)
            gate_proj = jnp.dot(group_mid, w_gate, preferred_element_type=jnp.float32)
            up_proj = jnp.dot(group_mid, w_up, preferred_element_type=jnp.float32)
            hidden_mlp = (jax.nn.silu(gate_proj) * up_proj).astype(jnp.bfloat16)
            mlp_part = jnp.dot(hidden_mlp, w_down, preferred_element_type=jnp.float32)
            summed = lax.psum_scatter(mlp_part, 'tp', scatter_dimension=0, tiled=True)
            outs.append((residual_mid[rows].astype(jnp.float32) + summed).astype(jnp.bfloat16))
        return jnp.concatenate(outs, axis=0)

    return jax.shard_map(device_layer, mesh=mesh, in_specs=(token_spec, P(('dp', 'cp', 'tp')), P('dp'), token_spec, token_spec, P(), column_spec, column_spec, column_spec, row_spec, P(), column_spec, column_spec, row_spec), out_specs=token_spec, check_vma=False)
```

```python
import functools
import math
import jax
import jax.numpy as jnp
from jax import lax
from jax.experimental import pallas as pl
from jax.experimental.pallas import tpu as pltpu
from jax.sharding import PartitionSpec as P

HEAD_DIM = 128
ROPE_BASE = 500000.0
NORM_EPS = 1e-5
RUN = 64
KV_BLOCK = 512
LOG2E = 1.4426950408889634


def rms_norm(hidden, norm_gain):
    values = hidden.astype(jnp.float32)
    inv_rms = lax.rsqrt(jnp.mean(values * values, axis=-1, keepdims=True) + NORM_EPS)
    return (values * inv_rms * norm_gain.astype(jnp.float32)).astype(jnp.bfloat16)


def rotary(projected, cos_table, sin_table):
    half_dim = HEAD_DIM // 2
    cos_table = cos_table[:, None, :]
    sin_table = sin_table[:, None, :]
    first_half = projected[..., :half_dim]
    second_half = projected[..., half_dim:]
    rotated = jnp.concatenate([first_half * cos_table - second_half * sin_table, second_half * cos_table + first_half * sin_table], axis=-1)
    return rotated.astype(jnp.bfloat16)


def attn_kernel(is_low, clen_ref, q_ref, kc_ref, vc_ref, knl_ref, vnl_ref, knh_ref, vnh_ref, o_ref, vt_ref, m_ref, l_ref, acc_ref):
    cp = lax.axis_index('cp')
    scale = LOG2E / math.sqrt(HEAD_DIM)
    half = q_ref.shape[0]
    slots = kc_ref.shape[0]
    fresh = knl_ref.shape[0]
    cache_len = clen_ref[0]

    @pl.when(pl.program_id(0) == 0)
    def _():
        for ref, base in ((vc_ref, 0), (vnl_ref, slots), (vnh_ref, slots + fresh))[:2 if is_low else 3]:
            for j in range(ref.shape[0] // 512):
                block = ref[j * 512:(j + 1) * 512, :].astype(jnp.float32)
                vt_ref[:, base + j * 512:base + (j + 1) * 512] = block.T.astype(jnp.bfloat16)

    m_ref[...] = jnp.full_like(m_ref, -1e30)
    l_ref[...] = jnp.zeros_like(l_ref)
    acc_ref[...] = jnp.zeros_like(acc_ref)

    def update(blocks):
        scores = []
        for keys, _, mask in blocks:
            raw = lax.dot_general(keys, q_ref[...], (((1,), (1,)), ((), ())), preferred_element_type=jnp.float32)
            scores.append(raw if mask is None else jnp.where(mask, raw, -jnp.inf))
        for (_, vt_cols, _), score in zip(blocks, scores):
            m_old = m_ref[...]
            m_new = jnp.maximum(m_old, jnp.max(score, axis=0, keepdims=True))
            probs = jnp.exp2((score - m_new) * scale)
            alpha = jnp.exp2((m_old - m_new) * scale)
            l_ref[...] = alpha * l_ref[...] + jnp.sum(probs, axis=0, keepdims=True)
            acc_ref[...] = alpha * acc_ref[...] + jnp.dot(vt_ref[:, vt_cols], probs.astype(jnp.bfloat16), preferred_element_type=jnp.float32)
            m_ref[...] = m_new

    def cache_block(start):
        rows = pl.ds(pl.multiple_of(start, KV_BLOCK), KV_BLOCK)
        visible = start + lax.broadcasted_iota(jnp.int32, (KV_BLOCK, half), 0) < cache_len
        return rows, visible

    full_pairs = cache_len // (2 * KV_BLOCK)

    def cache_step(j, carry):
        first, second = (cache_block(j * 2 * KV_BLOCK + i * KV_BLOCK)[0] for i in range(2))
        update([(kc_ref[first, :], first, None), (kc_ref[second, :], second, None)])
        return carry

    lax.fori_loop(0, full_pairs, cache_step, 0)

    def tail_step(j, carry):
        rows, visible = cache_block(j * KV_BLOCK)
        update([(kc_ref[rows, :], rows, visible)])
        return carry

    lax.fori_loop(2 * full_pairs, (cache_len + KV_BLOCK - 1) // KV_BLOCK, tail_step, 0)

    def new_keys(ref, base, j, mask=None):
        start = pl.multiple_of(j * half, half)
        return ref[pl.ds(start, half), :], pl.ds(pl.multiple_of(base + start, half), half), mask

    def low_step(j, carry):
        update([new_keys(knl_ref, slots, j)])
        return carry

    key_id = lax.broadcasted_iota(jnp.int32, (half, half), 0)
    row_id = lax.broadcasted_iota(jnp.int32, (half, half), 1)
    if is_low:
        lax.fori_loop(0, cp, low_step, 0)
        update([new_keys(knl_ref, slots, cp, key_id <= row_id)])
    else:
        for j in range(0, 4, 2):
            update([new_keys(knl_ref, slots, j), new_keys(knl_ref, slots, j + 1)])

        def high_step(j, carry):
            update([new_keys(knh_ref, slots + fresh, j)])
            return carry

        lax.fori_loop(cp + 1, 4, high_step, 0)
        runs = half // RUN

        def place(i):
            return (runs - 1 - i // RUN) * RUN + i % RUN

        update([new_keys(knh_ref, slots + fresh, cp, place(key_id) <= place(row_id))])
    o_ref[...] = (acc_ref[...] / l_ref[...]).T.astype(jnp.bfloat16)


def attention(cache_len, queries, cache_kv, low_kv, high_kv, is_low):
    rows, width = queries.shape
    heads = width // HEAD_DIM

    def column(array, index):
        return pl.BlockSpec((array.shape[0], HEAD_DIM), lambda g: (0, index))

    arrays = (cache_kv, low_kv, high_kv)
    return pl.pallas_call(
        functools.partial(attn_kernel, is_low),
        grid=(heads,),
        out_shape=jax.ShapeDtypeStruct((rows, width), jnp.bfloat16),
        in_specs=[pl.BlockSpec(memory_space=pltpu.SMEM), pl.BlockSpec((rows, HEAD_DIM), lambda g: (0, g))]
        + [column(a, i) for a in arrays for i in range(2)],
        out_specs=pl.BlockSpec((rows, HEAD_DIM), lambda g: (0, g)),
        scratch_shapes=[pltpu.VMEM((HEAD_DIM, sum(a.shape[0] for a in arrays)), jnp.bfloat16)] + [pltpu.VMEM((1, rows), jnp.float32)] * 2 + [pltpu.VMEM((HEAD_DIM, rows), jnp.float32)],
        cost_estimate=pl.CostEstimate(flops=2 * 2 * rows * width * 4608, bytes_accessed=8 * 2**20, transcendentals=rows * heads * 4608),
        name='attend',
    )(cache_len, queries, *[a for a in arrays for _ in range(2)])


def solution(mesh):
    tp_size, cp_size, dp_size = mesh.shape['tp'], mesh.shape['cp'], mesh.shape['dp']
    token_spec = P(('dp', 'cp', 'tp'), None)
    column_spec = P(None, 'tp')
    row_spec = P('tp', None)

    def device_layer(hidden_loc, pos_loc, cache_len, cache_k, cache_v, norm1_gain, w_query, w_key, w_value, w_out, norm2_gain, w_gate, w_up, w_down):
        _, d_model = hidden_loc.shape
        dp, tp, cp = lax.axis_index('dp'), lax.axis_index('tp'), lax.axis_index('cp')
        inv_freq = 1.0 / (ROPE_BASE ** (jnp.arange(HEAD_DIM // 2, dtype=jnp.float32) * (2.0 / HEAD_DIM)))

        def place(parts, me):
            size = len(parts)
            out = jnp.zeros((size,) + parts[0].shape, parts[0].dtype)
            for shift, part in enumerate(parts):
                out = lax.dynamic_update_index_in_dim(out, part, (me - shift) % size, 0)
            return out

        def shifted(part, axis_name, size, shift):
            return part if shift == 0 else lax.ppermute(part, axis_name, [(i, (i + shift) % size) for i in range(size)])

        def share(block):
            return place([shifted(block, 'cp', cp_size, shift) for shift in range(cp_size)], cp).reshape(-1, block.shape[-1])

        def exchange(block, split_axis):
            pieces = [lax.dynamic_index_in_dim(block, (tp + shift) % tp_size, split_axis, keepdims=False) for shift in range(tp_size)]
            return place([shifted(piece, 'tp', tp_size, shift) for shift, piece in enumerate(pieces)], tp)

        slots = cache_k.shape[0]
        cache_kv = jnp.stack([cache_k.reshape(slots, tp_size, HEAD_DIM), cache_v.reshape(slots, tp_size, HEAD_DIM)], axis=2)
        cache_kv = jnp.transpose(cache_kv.reshape(slots, tp_size, 2 * HEAD_DIM), (1, 0, 2))
        cache_kv = share(exchange(cache_kv, 0).reshape(tp_size * slots, 2 * HEAD_DIM))

        core, row_y = cp % 2, cp // 2
        column_width = d_model // tp_size
        piece_rows = w_out.shape[0] // (dp_size * cp_size)
        piece = lax.dynamic_slice_in_dim(w_out, (core * 4 + row_y * 2 + dp) * piece_rows, piece_rows, 0)
        columns = exchange(piece.reshape(piece_rows, tp_size, column_width), 1)
        for axis_name, size, flip, me in (('dp', dp_size, 1, dp), ('cp', cp_size, 2, row_y), ('cp', cp_size, 1, core)):
            columns = place([columns, lax.ppermute(columns, axis_name, [(i, i ^ flip) for i in range(size)])], me)
        columns = jnp.transpose(columns.reshape(dp_size * cp_size, tp_size, piece_rows, column_width), (1, 0, 2, 3))
        w_out_columns = columns.reshape(-1, column_width)

        gathered = [lax.all_gather(hidden_loc[i * RUN:(i + 1) * RUN], 'tp', axis=0, tiled=True) for i in range(2)]

        def project(index, rows_in):
            rows_in = rms_norm(rows_in, norm1_gain)
            runs = cp * tp_size + jnp.arange(tp_size)
            if index == 1:
                runs = 2 * cp_size * tp_size - 1 - runs
            positions = cache_len[0] + (runs[:, None] * RUN + jnp.arange(RUN)[None, :]).reshape(-1)
            angles = positions.astype(jnp.float32)[:, None] * inv_freq[None, :]
            cos_table, sin_table = jnp.cos(angles), jnp.sin(angles)

            def rotated(weight):
                wide = jnp.dot(rows_in, weight, preferred_element_type=jnp.float32).reshape(rows_in.shape[0], -1, HEAD_DIM)
                return rotary(wide, cos_table, sin_table).reshape(rows_in.shape[0], -1)

            values = jnp.dot(rows_in, w_value, preferred_element_type=jnp.float32).astype(jnp.bfloat16)
            return rotated(w_query), jnp.concatenate([rotated(w_key), values], axis=1)

        gathered[0], cache_kv, w_out_columns = lax.optimization_barrier((gathered[0], cache_kv, w_out_columns))
        q_low, low_kv = project(0, gathered[0])
        low_kv = share(low_kv)
        gathered[1], q_low, low_kv = lax.optimization_barrier((gathered[1], q_low, low_kv))
        q_high, high_kv = project(1, gathered[1])
        high_kv = share(high_kv)

        attended = [attention(cache_len, q_low, cache_kv, low_kv, high_kv, True)]
        q_high, attended[0] = lax.optimization_barrier((q_high, attended[0]))
        attended.append(attention(cache_len, q_high, cache_kv, low_kv, high_kv, False))
        column0 = tp * column_width
        outs = []
        for index in range(2):
            heads_all = lax.all_gather(attended[index], 'tp', axis=1, tiled=True)
            residual = lax.dynamic_slice_in_dim(gathered[index], column0, column_width, 1).astype(jnp.float32)
            mid = (residual + jnp.dot(heads_all, w_out_columns, preferred_element_type=jnp.float32)).astype(jnp.bfloat16)
            mid = lax.all_gather(mid, 'tp', axis=1, tiled=True)
            group_mid = rms_norm(mid, norm2_gain)
            gate_proj = jnp.dot(group_mid, w_gate, preferred_element_type=jnp.float32)
            up_proj = jnp.dot(group_mid, w_up, preferred_element_type=jnp.float32)
            hidden_mlp = (jax.nn.silu(gate_proj) * up_proj).astype(jnp.bfloat16)
            mlp_part = jnp.dot(hidden_mlp, w_down, preferred_element_type=jnp.float32)
            summed = lax.psum_scatter(mlp_part, 'tp', scatter_dimension=0, tiled=True)
            mine = lax.dynamic_slice_in_dim(mid, tp * RUN, RUN, 0)
            outs.append((mine.astype(jnp.float32) + summed).astype(jnp.bfloat16))
        return jnp.concatenate(outs, axis=0)

    return jax.shard_map(device_layer, mesh=mesh, in_specs=(token_spec, P(('dp', 'cp', 'tp')), P('dp'), token_spec, token_spec, P(), column_spec, column_spec, column_spec, row_spec, P(), column_spec, column_spec, row_spec), out_specs=token_spec, check_vma=False)
```

```python
import functools
import math
import jax
import jax.numpy as jnp
from jax import lax
from jax.experimental import pallas as pl
from jax.experimental.pallas import tpu as pltpu
from jax.sharding import PartitionSpec as P

HEAD_DIM = 128
ROPE_BASE = 500000.0
NORM_EPS = 1e-5
RUN = 64
KV_BLOCK = 512
LOG2E = 1.4426950408889634


def rms_norm(hidden, norm_gain):
    values = hidden.astype(jnp.float32)
    inv_rms = lax.rsqrt(jnp.mean(values * values, axis=-1, keepdims=True) + NORM_EPS)
    return (values * inv_rms * norm_gain.astype(jnp.float32)).astype(jnp.bfloat16)


def rotary(projected, cos_table, sin_table):
    half_dim = HEAD_DIM // 2
    cos_table = cos_table[:, None, :]
    sin_table = sin_table[:, None, :]
    first_half = projected[..., :half_dim]
    second_half = projected[..., half_dim:]
    rotated = jnp.concatenate([first_half * cos_table - second_half * sin_table, second_half * cos_table + first_half * sin_table], axis=-1)
    return rotated.astype(jnp.bfloat16)


def attn_kernel(is_low, clen_ref, q_ref, kc_ref, vc_ref, knl_ref, vnl_ref, knh_ref, vnh_ref, o_ref, vt_ref, m_ref, l_ref, acc_ref):
    cp = lax.axis_index('cp')
    scale = LOG2E / math.sqrt(HEAD_DIM)
    half = q_ref.shape[0]
    slots = kc_ref.shape[0]
    fresh = knl_ref.shape[0]
    cache_len = clen_ref[0]

    @pl.when(pl.program_id(0) == 0)
    def _():
        for ref, base in ((vc_ref, 0), (vnl_ref, slots), (vnh_ref, slots + fresh))[:2 if is_low else 3]:
            for j in range(ref.shape[0] // 512):
                block = ref[j * 512:(j + 1) * 512, :].astype(jnp.float32)
                vt_ref[:, base + j * 512:base + (j + 1) * 512] = block.T.astype(jnp.bfloat16)

    m_ref[...] = jnp.full_like(m_ref, -1e30)
    l_ref[...] = jnp.zeros_like(l_ref)
    acc_ref[...] = jnp.zeros_like(acc_ref)

    def update(blocks):
        scores = []
        for keys, _, mask in blocks:
            raw = lax.dot_general(keys, q_ref[...], (((1,), (1,)), ((), ())), preferred_element_type=jnp.float32)
            scores.append(raw if mask is None else jnp.where(mask, raw, -jnp.inf))
        for (_, vt_cols, _), score in zip(blocks, scores):
            m_old = m_ref[...]
            m_new = jnp.maximum(m_old, jnp.max(score, axis=0, keepdims=True))
            probs = jnp.exp2((score - m_new) * scale)
            alpha = jnp.exp2((m_old - m_new) * scale)
            l_ref[...] = alpha * l_ref[...] + jnp.sum(probs, axis=0, keepdims=True)
            acc_ref[...] = alpha * acc_ref[...] + jnp.dot(vt_ref[:, vt_cols], probs.astype(jnp.bfloat16), preferred_element_type=jnp.float32)
            m_ref[...] = m_new

    def cache_block(start):
        rows = pl.ds(pl.multiple_of(start, KV_BLOCK), KV_BLOCK)
        visible = start + lax.broadcasted_iota(jnp.int32, (KV_BLOCK, half), 0) < cache_len
        return rows, visible

    full_pairs = cache_len // (2 * KV_BLOCK)

    def cache_step(j, carry):
        first, second = (cache_block(j * 2 * KV_BLOCK + i * KV_BLOCK)[0] for i in range(2))
        update([(kc_ref[first, :], first, None), (kc_ref[second, :], second, None)])
        return carry

    lax.fori_loop(0, full_pairs, cache_step, 0)

    def tail_step(j, carry):
        rows, visible = cache_block(j * KV_BLOCK)
        update([(kc_ref[rows, :], rows, visible)])
        return carry

    lax.fori_loop(2 * full_pairs, (cache_len + KV_BLOCK - 1) // KV_BLOCK, tail_step, 0)

    def new_keys(ref, base, j, mask=None):
        start = pl.multiple_of(j * half, half)
        return ref[pl.ds(start, half), :], pl.ds(pl.multiple_of(base + start, half), half), mask

    def low_step(j, carry):
        update([new_keys(knl_ref, slots, j)])
        return carry

    key_id = lax.broadcasted_iota(jnp.int32, (half, half), 0)
    row_id = lax.broadcasted_iota(jnp.int32, (half, half), 1)
    if is_low:
        lax.fori_loop(0, cp, low_step, 0)
        update([new_keys(knl_ref, slots, cp, key_id <= row_id)])
    else:
        for j in range(0, 4, 2):
            update([new_keys(knl_ref, slots, j), new_keys(knl_ref, slots, j + 1)])

        def high_step(j, carry):
            update([new_keys(knh_ref, slots + fresh, j)])
            return carry

        lax.fori_loop(cp + 1, 4, high_step, 0)
        runs = half // RUN

        def place(i):
            return (runs - 1 - i // RUN) * RUN + i % RUN

        update([new_keys(knh_ref, slots + fresh, cp, place(key_id) <= place(row_id))])
    o_ref[...] = (acc_ref[...] / l_ref[...]).T.astype(jnp.bfloat16)


def attention(cache_len, queries, cache_kv, low_kv, high_kv, is_low, head0, heads):
    rows = queries.shape[0]
    width = heads * HEAD_DIM

    def column(array, index):
        return pl.BlockSpec((array.shape[0], HEAD_DIM), lambda g: (0, index))

    arrays = (cache_kv, low_kv, high_kv)
    return pl.pallas_call(
        functools.partial(attn_kernel, is_low),
        grid=(heads,),
        out_shape=jax.ShapeDtypeStruct((rows, width), jnp.bfloat16),
        in_specs=[pl.BlockSpec(memory_space=pltpu.SMEM), pl.BlockSpec((rows, HEAD_DIM), lambda g: (0, g + head0))]
        + [column(a, i) for a in arrays for i in range(2)],
        out_specs=pl.BlockSpec((rows, HEAD_DIM), lambda g: (0, g)),
        scratch_shapes=[pltpu.VMEM((HEAD_DIM, sum(a.shape[0] for a in arrays)), jnp.bfloat16)] + [pltpu.VMEM((1, rows), jnp.float32)] * 2 + [pltpu.VMEM((HEAD_DIM, rows), jnp.float32)],
        cost_estimate=pl.CostEstimate(flops=2 * 2 * rows * width * 4608, bytes_accessed=8 * 2**20, transcendentals=rows * heads * 4608),
        name='attend',
    )(cache_len, queries, *[a for a in arrays for _ in range(2)])


def solution(mesh):
    tp_size, cp_size, dp_size = mesh.shape['tp'], mesh.shape['cp'], mesh.shape['dp']
    token_spec = P(('dp', 'cp', 'tp'), None)
    column_spec = P(None, 'tp')
    row_spec = P('tp', None)

    def layer(hidden_loc, pos_loc, cache_len, cache_k, cache_v, norm1_gain, w_query, w_key, w_value, w_out, norm2_gain, w_gate, w_up, w_down):
        _, d_model = hidden_loc.shape
        dp, tp, cp = lax.axis_index('dp'), lax.axis_index('tp'), lax.axis_index('cp')
        inv_freq = 1.0 / (ROPE_BASE ** (jnp.arange(HEAD_DIM // 2, dtype=jnp.float32) * (2.0 / HEAD_DIM)))

        def place(parts, me):
            size = len(parts)
            out = jnp.zeros((size,) + parts[0].shape, parts[0].dtype)
            for shift, part in enumerate(parts):
                out = lax.dynamic_update_index_in_dim(out, part, (me - shift) % size, 0)
            return out

        def shifted(part, axis_name, size, shift):
            return part if shift == 0 else lax.ppermute(part, axis_name, [(i, (i + shift) % size) for i in range(size)])

        def share(block):
            return place([shifted(block, 'cp', cp_size, shift) for shift in range(cp_size)], cp).reshape(-1, block.shape[-1])

        def exchange(block, split_axis):
            pieces = [lax.dynamic_index_in_dim(block, (tp + shift) % tp_size, split_axis, keepdims=False) for shift in range(tp_size)]
            return place([shifted(piece, 'tp', tp_size, shift) for shift, piece in enumerate(pieces)], tp)

        gathered = []
        for i in range(2):
            gathered.append(lax.all_gather(hidden_loc[i * RUN:(i + 1) * RUN], 'tp', axis=0, tiled=True))

        slots = cache_k.shape[0]
        cache_kv = jnp.stack([cache_k.reshape(slots, tp_size, HEAD_DIM), cache_v.reshape(slots, tp_size, HEAD_DIM)], axis=2)
        cache_kv = jnp.transpose(cache_kv.reshape(slots, tp_size, 2 * HEAD_DIM), (1, 0, 2))
        cache_kv = exchange(cache_kv, 0).reshape(tp_size * slots, 2 * HEAD_DIM)
        cache_kv = share(cache_kv)

        column_width = d_model // cp_size

        def flipped(part, flip, axis_name='cp', size=cp_size):
            return part if flip == 0 else lax.ppermute(part, axis_name, [(i, i ^ flip) for i in range(size)])

        def columns_of(array, flip):
            return lax.dynamic_slice_in_dim(array, (cp ^ flip) * column_width, column_width, 1)

        residual_columns = [flipped(columns_of(hidden_loc, flip), flip) for flip in range(cp_size)]

        def project(index, rows_in):
            rows_in = rms_norm(rows_in, norm1_gain)
            runs = cp * tp_size + jnp.arange(tp_size)
            if index == 1:
                runs = 2 * cp_size * tp_size - 1 - runs
            positions = cache_len[0] + (runs[:, None] * RUN + jnp.arange(RUN)[None, :]).reshape(-1)
            angles = positions.astype(jnp.float32)[:, None] * inv_freq[None, :]
            cos_table, sin_table = jnp.cos(angles), jnp.sin(angles)

            def rotated(weight):
                wide = jnp.dot(rows_in, weight, preferred_element_type=jnp.float32).reshape(rows_in.shape[0], -1, HEAD_DIM)
                return rotary(wide, cos_table, sin_table).reshape(rows_in.shape[0], -1)

            values = jnp.dot(rows_in, w_value, preferred_element_type=jnp.float32).astype(jnp.bfloat16)
            return rotated(w_query), jnp.concatenate([rotated(w_key), values], axis=1)

        gathered[0], cache_kv = lax.optimization_barrier((gathered[0], cache_kv))
        q_low, low_kv = project(0, gathered[0])
        low_kv = share(low_kv)
        gathered[1], q_low, low_kv, residual_columns = lax.optimization_barrier((gathered[1], q_low, low_kv, residual_columns))
        q_high, high_kv = project(1, gathered[1])
        high_kv = share(high_kv)

        w_out_local = columns_of(w_out, 0)
        half_rows = w_out.shape[0] // dp_size
        w_half = lax.dynamic_slice_in_dim(w_out_local, dp * half_rows, half_rows, 0)
        w_half, high_kv, q_high = lax.optimization_barrier((w_half, high_kv, q_high))
        w_halves = [shifted(w_half, 'tp', tp_size, shift) for shift in range(1, tp_size)]
        low_out = attention(cache_len, q_low, cache_kv, low_kv, high_kv, True, 0, 7)

        def to_owner(out):
            blocks = out.reshape(tp_size, RUN, out.shape[1])
            return [shifted(lax.dynamic_index_in_dim(blocks, (tp + shift) % tp_size, 0, keepdims=False), 'tp', tp_size, shift) for shift in range(tp_size)]

        low_parts = to_owner(low_out)
        q_high, low_out, w_halves = lax.optimization_barrier((q_high, low_out, w_halves))
        w_others = [flipped(w, 1, 'dp', dp_size) for w in w_halves]
        high_a = attention(cache_len, q_high, cache_kv, low_kv, high_kv, False, 0, 4)
        high_parts_a = to_owner(high_a)

        def spread(parts):
            block = jnp.stack(parts)
            across = flipped(block, 2)
            return [block, flipped(block, 1), across, flipped(across, 1)]

        low_parts, q_high = lax.optimization_barrier((low_parts, q_high))
        low_rows = spread(low_parts)
        high_b = attention(cache_len, q_high, cache_kv, low_kv, high_kv, False, 4, 3)
        high_parts_b = to_owner(high_b)
        high_parts = [jnp.concatenate(pair, axis=1) for pair in zip(high_parts_a, high_parts_b)]
        high_rows = spread(high_parts)
        w_all = [w_out_local] + [jnp.where(dp == 0, jnp.concatenate([w, o], axis=0), jnp.concatenate([o, w], axis=0)) for w, o in zip(w_halves, w_others)]

        outs = []
        for index, spread_rows in enumerate((low_rows, high_rows)):
            rows = slice(index * RUN, (index + 1) * RUN)
            rows_in = jnp.concatenate(spread_rows, axis=1)
            attn_out = sum(jnp.dot(rows_in[shift], w_all[shift], preferred_element_type=jnp.float32) for shift in range(tp_size))
            mid_columns = (jnp.concatenate([r[rows] for r in residual_columns], axis=0).astype(jnp.float32) + attn_out).astype(jnp.bfloat16)
            mid = jnp.zeros((RUN, cp_size, column_width), jnp.bfloat16)
            for flip in range(cp_size):
                part = flipped(mid_columns[flip * RUN:(flip + 1) * RUN], flip)
                mid = lax.dynamic_update_slice_in_dim(mid, part[:, None, :], cp ^ flip, 1)
            mid = mid.reshape(RUN, d_model)
            group_mid = lax.all_gather(rms_norm(mid, norm2_gain), 'tp', axis=0, tiled=True)
            gate_proj = jnp.dot(group_mid, w_gate, preferred_element_type=jnp.float32)
            up_proj = jnp.dot(group_mid, w_up, preferred_element_type=jnp.float32)
            hidden_mlp = (jax.nn.silu(gate_proj) * up_proj).astype(jnp.bfloat16)
            mlp_part = jnp.dot(hidden_mlp, w_down, preferred_element_type=jnp.float32)
            summed = lax.psum_scatter(mlp_part, 'tp', scatter_dimension=0, tiled=True)
            outs.append((mid.astype(jnp.float32) + summed).astype(jnp.bfloat16))
        return jnp.concatenate(outs, axis=0)

    return jax.shard_map(layer, mesh=mesh, in_specs=(token_spec, P(('dp', 'cp', 'tp')), P('dp'), token_spec, token_spec, P(), column_spec, column_spec, column_spec, row_spec, P(), column_spec, column_spec, row_spec), out_specs=token_spec, check_vma=False)
```

```python
import functools
import math
import jax
import jax.numpy as jnp
from jax import lax
from jax.experimental import pallas as pl
from jax.experimental.pallas import tpu as pltpu
from jax.sharding import PartitionSpec as P

HEAD_DIM = 128
ROPE_BASE = 500000.0
NORM_EPS = 1e-5
RUN = 64
KV_BLOCK = 512
LOG2E = 1.4426950408889634


def rms_norm(hidden, norm_gain):
    values = hidden.astype(jnp.float32)
    inv_rms = lax.rsqrt(jnp.mean(values * values, axis=-1, keepdims=True) + NORM_EPS)
    return (values * inv_rms * norm_gain.astype(jnp.float32)).astype(jnp.bfloat16)


def rotary(projected, cos_table, sin_table):
    half_dim = HEAD_DIM // 2
    cos_table = cos_table[:, None, :]
    sin_table = sin_table[:, None, :]
    first_half = projected[..., :half_dim]
    second_half = projected[..., half_dim:]
    rotated = jnp.concatenate([first_half * cos_table - second_half * sin_table, second_half * cos_table + first_half * sin_table], axis=-1)
    return rotated.astype(jnp.bfloat16)


def attn_kernel(is_low, clen_ref, q_ref, kc_ref, vc_ref, knl_ref, vnl_ref, knh_ref, vnh_ref, o_ref, vt_ref, m_ref, l_ref, acc_ref):
    cp = lax.axis_index('cp')
    scale = LOG2E / math.sqrt(HEAD_DIM)
    half = q_ref.shape[0]
    slots = kc_ref.shape[0]
    fresh = knl_ref.shape[0]
    cache_len = clen_ref[0]

    @pl.when(pl.program_id(0) == 0)
    def _():
        for ref, base in ((vc_ref, 0), (vnl_ref, slots), (vnh_ref, slots + fresh))[:2 if is_low else 3]:
            for j in range(ref.shape[0] // 512):
                block = ref[j * 512:(j + 1) * 512, :].astype(jnp.float32)
                vt_ref[:, base + j * 512:base + (j + 1) * 512] = block.T.astype(jnp.bfloat16)

    m_ref[...] = jnp.full_like(m_ref, -1e30)
    l_ref[...] = jnp.zeros_like(l_ref)
    acc_ref[...] = jnp.zeros_like(acc_ref)

    def update(blocks):
        scores = []
        for keys, _, mask in blocks:
            raw = lax.dot_general(keys, q_ref[...], (((1,), (1,)), ((), ())), preferred_element_type=jnp.float32)
            scores.append(raw if mask is None else jnp.where(mask, raw, -jnp.inf))
        for (_, vt_cols, _), score in zip(blocks, scores):
            m_old = m_ref[...]
            m_new = jnp.maximum(m_old, jnp.max(score, axis=0, keepdims=True))
            probs = jnp.exp2((score - m_new) * scale)
            alpha = jnp.exp2((m_old - m_new) * scale)
            l_ref[...] = alpha * l_ref[...] + jnp.sum(probs, axis=0, keepdims=True)
            acc_ref[...] = alpha * acc_ref[...] + jnp.dot(vt_ref[:, vt_cols], probs.astype(jnp.bfloat16), preferred_element_type=jnp.float32)
            m_ref[...] = m_new

    def cache_block(start):
        rows = pl.ds(pl.multiple_of(start, KV_BLOCK), KV_BLOCK)
        visible = start + lax.broadcasted_iota(jnp.int32, (KV_BLOCK, half), 0) < cache_len
        return rows, visible

    full_pairs = cache_len // (2 * KV_BLOCK)

    def cache_step(j, carry):
        first, second = (cache_block(j * 2 * KV_BLOCK + i * KV_BLOCK)[0] for i in range(2))
        update([(kc_ref[first, :], first, None), (kc_ref[second, :], second, None)])
        return carry

    lax.fori_loop(0, full_pairs, cache_step, 0)

    def tail_step(j, carry):
        rows, visible = cache_block(j * KV_BLOCK)
        update([(kc_ref[rows, :], rows, visible)])
        return carry

    lax.fori_loop(2 * full_pairs, (cache_len + KV_BLOCK - 1) // KV_BLOCK, tail_step, 0)

    def new_keys(ref, base, j, mask=None):
        start = pl.multiple_of(j * half, half)
        return ref[pl.ds(start, half), :], pl.ds(pl.multiple_of(base + start, half), half), mask

    def low_step(j, carry):
        update([new_keys(knl_ref, slots, j)])
        return carry

    key_id = lax.broadcasted_iota(jnp.int32, (half, half), 0)
    row_id = lax.broadcasted_iota(jnp.int32, (half, half), 1)
    if is_low:
        lax.fori_loop(0, cp, low_step, 0)
        update([new_keys(knl_ref, slots, cp, key_id <= row_id)])
    else:
        for j in range(0, 4, 2):
            update([new_keys(knl_ref, slots, j), new_keys(knl_ref, slots, j + 1)])

        def high_step(j, carry):
            update([new_keys(knh_ref, slots + fresh, j)])
            return carry

        lax.fori_loop(cp + 1, 4, high_step, 0)
        runs = half // RUN

        def place(i):
            return (runs - 1 - i // RUN) * RUN + i % RUN

        update([new_keys(knh_ref, slots + fresh, cp, place(key_id) <= place(row_id))])
    o_ref[...] = (acc_ref[...] / l_ref[...]).T.astype(jnp.bfloat16)


def attention(cache_len, queries, cache_kv, low_kv, high_kv, is_low, head0, heads):
    rows = queries.shape[0]
    width = heads * HEAD_DIM

    def column(array, index):
        return pl.BlockSpec((array.shape[0], HEAD_DIM), lambda g: (0, index))

    arrays = (cache_kv, low_kv, high_kv)
    return pl.pallas_call(
        functools.partial(attn_kernel, is_low),
        grid=(heads,),
        out_shape=jax.ShapeDtypeStruct((rows, width), jnp.bfloat16),
        in_specs=[pl.BlockSpec(memory_space=pltpu.SMEM), pl.BlockSpec((rows, HEAD_DIM), lambda g: (0, g + head0))]
        + [column(a, i) for a in arrays for i in range(2)],
        out_specs=pl.BlockSpec((rows, HEAD_DIM), lambda g: (0, g)),
        scratch_shapes=[pltpu.VMEM((HEAD_DIM, sum(a.shape[0] for a in arrays)), jnp.bfloat16)] + [pltpu.VMEM((1, rows), jnp.float32)] * 2 + [pltpu.VMEM((HEAD_DIM, rows), jnp.float32)],
        cost_estimate=pl.CostEstimate(flops=2 * 2 * rows * width * 4608, bytes_accessed=8 * 2**20, transcendentals=rows * heads * 4608),
        name='attend',
    )(cache_len, queries, *[a for a in arrays for _ in range(2)])


def solution(mesh):
    tp_size, cp_size, dp_size = mesh.shape['tp'], mesh.shape['cp'], mesh.shape['dp']
    token_spec = P(('dp', 'cp', 'tp'), None)
    column_spec = P(None, 'tp')
    row_spec = P('tp', None)

    def layer(hidden_loc, pos_loc, cache_len, cache_k, cache_v, norm1_gain, w_query, w_key, w_value, w_out, norm2_gain, w_gate, w_up, w_down):
        _, d_model = hidden_loc.shape
        dp, tp, cp = lax.axis_index('dp'), lax.axis_index('tp'), lax.axis_index('cp')
        inv_freq = 1.0 / (ROPE_BASE ** (jnp.arange(HEAD_DIM // 2, dtype=jnp.float32) * (2.0 / HEAD_DIM)))

        def place(parts, me):
            size = len(parts)
            out = jnp.zeros((size,) + parts[0].shape, parts[0].dtype)
            for shift, part in enumerate(parts):
                out = lax.dynamic_update_index_in_dim(out, part, (me - shift) % size, 0)
            return out

        def shifted(part, axis_name, size, shift):
            return part if shift == 0 else lax.ppermute(part, axis_name, [(i, (i + shift) % size) for i in range(size)])

        def share(block):
            return place([shifted(block, 'cp', cp_size, shift) for shift in range(cp_size)], cp).reshape(-1, block.shape[-1])

        def exchange(block, split_axis):
            pieces = [lax.dynamic_index_in_dim(block, (tp + shift) % tp_size, split_axis, keepdims=False) for shift in range(tp_size)]
            return place([shifted(piece, 'tp', tp_size, shift) for shift, piece in enumerate(pieces)], tp)

        def gather_rows(block, after=None):
            parts = [shifted(block, 'tp', tp_size, shift) for shift in range(tp_size)]
            if after is not None:
                parts = lax.optimization_barrier((parts, after))[0]
            return place(parts, tp).reshape(-1, d_model)

        gathered = [lax.all_gather(hidden_loc[:RUN], 'tp', axis=0, tiled=True)]
        gathered.append(gather_rows(hidden_loc[RUN:]))

        slots = cache_k.shape[0]
        cache_kv = jnp.stack([cache_k.reshape(slots, tp_size, HEAD_DIM), cache_v.reshape(slots, tp_size, HEAD_DIM)], axis=2)
        cache_kv = jnp.transpose(cache_kv.reshape(slots, tp_size, 2 * HEAD_DIM), (1, 0, 2))
        cache_kv = exchange(cache_kv, 0).reshape(tp_size * slots, 2 * HEAD_DIM)
        cache_kv = share(cache_kv)

        column_width = d_model // cp_size

        def flipped(part, flip, axis_name='cp', size=cp_size):
            return part if flip == 0 else lax.ppermute(part, axis_name, [(i, i ^ flip) for i in range(size)])

        def columns_of(array, flip):
            return lax.dynamic_slice_in_dim(array, (cp ^ flip) * column_width, column_width, 1)

        residual_columns = [flipped(columns_of(hidden_loc, flip), flip) for flip in range(cp_size)]

        def project(index, rows_in):
            rows_in = rms_norm(rows_in, norm1_gain)
            runs = cp * tp_size + jnp.arange(tp_size)
            if index == 1:
                runs = 2 * cp_size * tp_size - 1 - runs
            positions = cache_len[0] + (runs[:, None] * RUN + jnp.arange(RUN)[None, :]).reshape(-1)
            angles = positions.astype(jnp.float32)[:, None] * inv_freq[None, :]
            cos_table, sin_table = jnp.cos(angles), jnp.sin(angles)

            def rotated(weight):
                wide = jnp.dot(rows_in, weight, preferred_element_type=jnp.float32).reshape(rows_in.shape[0], -1, HEAD_DIM)
                return rotary(wide, cos_table, sin_table).reshape(rows_in.shape[0], -1)

            values = jnp.dot(rows_in, w_value, preferred_element_type=jnp.float32).astype(jnp.bfloat16)
            return rotated(w_query), jnp.concatenate([rotated(w_key), values], axis=1)

        gathered[0], cache_kv = lax.optimization_barrier((gathered[0], cache_kv))
        q_low, low_kv = project(0, gathered[0])
        low_kv = share(low_kv)
        gathered[1], q_low, low_kv, residual_columns = lax.optimization_barrier((gathered[1], q_low, low_kv, residual_columns))
        q_high, high_kv = project(1, gathered[1])
        high_kv = share(high_kv)

        w_out_local = columns_of(w_out, 0)
        half_rows = w_out.shape[0] // dp_size
        w_half = lax.dynamic_slice_in_dim(w_out_local, dp * half_rows, half_rows, 0)
        w_halves = [shifted(w_half, 'tp', tp_size, shift) for shift in range(1, tp_size)]
        low_out = attention(cache_len, q_low, cache_kv, low_kv, high_kv, True, 0, 7)

        def to_owner(out):
            blocks = out.reshape(tp_size, RUN, out.shape[1])
            return [shifted(lax.dynamic_index_in_dim(blocks, (tp + shift) % tp_size, 0, keepdims=False), 'tp', tp_size, shift) for shift in range(tp_size)]

        low_parts = to_owner(low_out)
        q_high, low_out = lax.optimization_barrier((q_high, low_out))
        w_others = [flipped(w, 1, 'dp', dp_size) for w in w_halves]
        high_a = attention(cache_len, q_high, cache_kv, low_kv, high_kv, False, 0, 4)
        high_parts_a = to_owner(high_a)

        def spread(parts):
            block = jnp.stack(parts)
            across = flipped(block, 2)
            return [block, flipped(block, 1), across, flipped(across, 1)]

        low_parts, q_high = lax.optimization_barrier((low_parts, q_high))
        low_rows = spread(low_parts)
        high_b = attention(cache_len, q_high, cache_kv, low_kv, high_kv, False, 4, 3)
        high_parts_b = to_owner(high_b)
        high_parts = [jnp.concatenate(pair, axis=1) for pair in zip(high_parts_a, high_parts_b)]
        high_rows = spread(high_parts)
        w_all = [w_out_local] + [jnp.where(dp == 0, jnp.concatenate([w, o], axis=0), jnp.concatenate([o, w], axis=0)) for w, o in zip(w_halves, w_others)]

        outs = []
        group_mid = None
        for index, spread_rows in enumerate((low_rows, high_rows)):
            rows = slice(index * RUN, (index + 1) * RUN)
            rows_in = jnp.concatenate(spread_rows, axis=1)
            attn_out = sum(jnp.dot(rows_in[shift], w_all[shift], preferred_element_type=jnp.float32) for shift in range(tp_size))
            mid_columns = (jnp.concatenate([r[rows] for r in residual_columns], axis=0).astype(jnp.float32) + attn_out).astype(jnp.bfloat16)
            mid = jnp.zeros((RUN, cp_size, column_width), jnp.bfloat16)
            for flip in range(cp_size):
                part = flipped(mid_columns[flip * RUN:(flip + 1) * RUN], flip)
                mid = lax.dynamic_update_slice_in_dim(mid, part[:, None, :], cp ^ flip, 1)
            mid = mid.reshape(RUN, d_model)
            normed_mid = rms_norm(mid, norm2_gain)
            for start, count in (((0, RUN // 2), (RUN // 2, RUN // 2)), ((0, RUN),))[index]:
                group_mid = gather_rows(normed_mid[start:start + count], group_mid)
                gate_proj = jnp.dot(group_mid, w_gate, preferred_element_type=jnp.float32)
                up_proj = jnp.dot(group_mid, w_up, preferred_element_type=jnp.float32)
                hidden_mlp = (jax.nn.silu(gate_proj) * up_proj).astype(jnp.bfloat16)
                mlp_part = jnp.dot(hidden_mlp, w_down, preferred_element_type=jnp.float32)
                summed = lax.psum_scatter(mlp_part, 'tp', scatter_dimension=0, tiled=True)
                outs.append((mid[start:start + count].astype(jnp.float32) + summed).astype(jnp.bfloat16))
        return jnp.concatenate(outs, axis=0)

    return jax.shard_map(layer, mesh=mesh, in_specs=(token_spec, P(('dp', 'cp', 'tp')), P('dp'), token_spec, token_spec, P(), column_spec, column_spec, column_spec, row_spec, P(), column_spec, column_spec, row_spec), out_specs=token_spec, check_vma=False)
```

```python
import functools
import math
import jax
import jax.numpy as jnp
from jax import lax
from jax.experimental import pallas as pl
from jax.experimental.pallas import tpu as pltpu
from jax.sharding import PartitionSpec as P

HEAD_DIM = 128
ROPE_BASE = 500000.0
NORM_EPS = 1e-5
RUN = 64
KV_BLOCK = 512
MLP_TILE = 512
LOG2E = 1.4426950408889634


def rms_norm(hidden, norm_gain):
    values = hidden.astype(jnp.float32)
    inv_rms = lax.rsqrt(jnp.mean(values * values, axis=-1, keepdims=True) + NORM_EPS)
    return (values * inv_rms * norm_gain.astype(jnp.float32)).astype(jnp.bfloat16)


def rotary(projected, cos_table, sin_table):
    half_dim = HEAD_DIM // 2
    cos_table = cos_table[:, None, :]
    sin_table = sin_table[:, None, :]
    first_half = projected[..., :half_dim]
    second_half = projected[..., half_dim:]
    rotated = jnp.concatenate([first_half * cos_table - second_half * sin_table, second_half * cos_table + first_half * sin_table], axis=-1)
    return rotated.astype(jnp.bfloat16)


def attn_kernel(is_low, clen_ref, q_ref, kc_ref, vc_ref, knl_ref, vnl_ref, knh_ref, vnh_ref, o_ref, vt_ref, m_ref, l_ref, acc_ref):
    cp = lax.axis_index('cp')
    scale = LOG2E / math.sqrt(HEAD_DIM)
    half = q_ref.shape[0]
    slots = kc_ref.shape[0]
    fresh = knl_ref.shape[0]
    cache_len = clen_ref[0]

    @pl.when(pl.program_id(0) == 0)
    def _():
        for ref, base in ((vc_ref, 0), (vnl_ref, slots), (vnh_ref, slots + fresh))[:2 if is_low else 3]:
            for j in range(ref.shape[0] // 512):
                block = ref[j * 512:(j + 1) * 512, :].astype(jnp.float32)
                vt_ref[:, base + j * 512:base + (j + 1) * 512] = block.T.astype(jnp.bfloat16)

    m_ref[...] = jnp.full_like(m_ref, -1e30)
    l_ref[...] = jnp.zeros_like(l_ref)
    acc_ref[...] = jnp.zeros_like(acc_ref)

    def update(blocks):
        scores = []
        for keys, _, mask in blocks:
            raw = lax.dot_general(keys, q_ref[...], (((1,), (1,)), ((), ())), preferred_element_type=jnp.float32)
            scores.append(raw if mask is None else jnp.where(mask, raw, -jnp.inf))
        for (_, vt_cols, _), score in zip(blocks, scores):
            m_old = m_ref[...]
            m_new = jnp.maximum(m_old, jnp.max(score, axis=0, keepdims=True))
            probs = jnp.exp2((score - m_new) * scale)
            alpha = jnp.exp2((m_old - m_new) * scale)
            l_ref[...] = alpha * l_ref[...] + jnp.sum(probs, axis=0, keepdims=True)
            acc_ref[...] = alpha * acc_ref[...] + jnp.dot(vt_ref[:, vt_cols], probs.astype(jnp.bfloat16), preferred_element_type=jnp.float32)
            m_ref[...] = m_new

    def cache_block(start):
        rows = pl.ds(pl.multiple_of(start, KV_BLOCK), KV_BLOCK)
        visible = start + lax.broadcasted_iota(jnp.int32, (KV_BLOCK, half), 0) < cache_len
        return rows, visible

    full_pairs = cache_len // (2 * KV_BLOCK)

    def cache_step(j, carry):
        first, second = (cache_block(j * 2 * KV_BLOCK + i * KV_BLOCK)[0] for i in range(2))
        update([(kc_ref[first, :], first, None), (kc_ref[second, :], second, None)])
        return carry

    lax.fori_loop(0, full_pairs, cache_step, 0)

    def tail_step(j, carry):
        rows, visible = cache_block(j * KV_BLOCK)
        update([(kc_ref[rows, :], rows, visible)])
        return carry

    lax.fori_loop(2 * full_pairs, (cache_len + KV_BLOCK - 1) // KV_BLOCK, tail_step, 0)

    def new_keys(ref, base, j, mask=None):
        start = pl.multiple_of(j * half, half)
        return ref[pl.ds(start, half), :], pl.ds(pl.multiple_of(base + start, half), half), mask

    def low_step(j, carry):
        update([new_keys(knl_ref, slots, j)])
        return carry

    key_id = lax.broadcasted_iota(jnp.int32, (half, half), 0)
    row_id = lax.broadcasted_iota(jnp.int32, (half, half), 1)
    if is_low:
        lax.fori_loop(0, cp, low_step, 0)
        update([new_keys(knl_ref, slots, cp, key_id <= row_id)])
    else:
        for j in range(0, 4, 2):
            update([new_keys(knl_ref, slots, j), new_keys(knl_ref, slots, j + 1)])

        def high_step(j, carry):
            update([new_keys(knh_ref, slots + fresh, j)])
            return carry

        lax.fori_loop(cp + 1, 4, high_step, 0)
        runs = half // RUN

        def place(i):
            return (runs - 1 - i // RUN) * RUN + i % RUN

        update([new_keys(knh_ref, slots + fresh, cp, place(key_id) <= place(row_id))])
    o_ref[...] = (acc_ref[...] / l_ref[...]).T.astype(jnp.bfloat16)


def attention(cache_len, queries, cache_kv, low_kv, high_kv, is_low, head0, heads):
    rows = queries.shape[0]
    width = heads * HEAD_DIM

    def column(array, index):
        return pl.BlockSpec((array.shape[0], HEAD_DIM), lambda g: (0, index))

    arrays = (cache_kv, low_kv, high_kv)
    return pl.pallas_call(
        functools.partial(attn_kernel, is_low),
        grid=(heads,),
        out_shape=jax.ShapeDtypeStruct((rows, width), jnp.bfloat16),
        in_specs=[pl.BlockSpec(memory_space=pltpu.SMEM), pl.BlockSpec((rows, HEAD_DIM), lambda g: (0, g + head0))]
        + [column(a, i) for a in arrays for i in range(2)],
        out_specs=pl.BlockSpec((rows, HEAD_DIM), lambda g: (0, g)),
        scratch_shapes=[pltpu.VMEM((HEAD_DIM, sum(a.shape[0] for a in arrays)), jnp.bfloat16)] + [pltpu.VMEM((1, rows), jnp.float32)] * 2 + [pltpu.VMEM((HEAD_DIM, rows), jnp.float32)],
        cost_estimate=pl.CostEstimate(flops=2 * 2 * rows * width * 4608, bytes_accessed=8 * 2**20, transcendentals=rows * heads * 4608),
        name='attend',
    )(cache_len, queries, *[a for a in arrays for _ in range(2)])


def mlp_kernel(tail, rows_ref, gate_ref, up_ref, down_ref, out_ref):
    step = pl.program_id(0)
    last = pl.num_programs(0) - 1

    @pl.when(step == 0)
    def _():
        out_ref[...] = jnp.zeros_like(out_ref)

    def tile(width):
        rows = rows_ref[...]
        gate_proj = jnp.dot(rows, gate_ref[:, :width], preferred_element_type=jnp.float32)
        up_proj = jnp.dot(rows, up_ref[:, :width], preferred_element_type=jnp.float32)
        hidden_mlp = (jax.nn.silu(gate_proj) * up_proj).astype(jnp.bfloat16)
        out_ref[...] += jnp.dot(hidden_mlp, down_ref[:width, :], preferred_element_type=jnp.float32)

    @pl.when(step < last)
    def _():
        tile(gate_ref.shape[1])

    @pl.when(step == last)
    def _():
        tile(tail)


def gated_mlp(rows, w_gate, w_up, w_down):
    count, d_model = rows.shape
    width = w_gate.shape[1]
    steps = (width + MLP_TILE - 1) // MLP_TILE
    wide = pl.BlockSpec((d_model, MLP_TILE), lambda i: (0, i))
    return pl.pallas_call(
        functools.partial(mlp_kernel, width - (steps - 1) * MLP_TILE),
        grid=(steps,),
        out_shape=jax.ShapeDtypeStruct((count, d_model), jnp.float32),
        in_specs=[pl.BlockSpec((count, d_model), lambda i: (0, 0)), wide, wide, pl.BlockSpec((MLP_TILE, d_model), lambda i: (i, 0))],
        out_specs=pl.BlockSpec((count, d_model), lambda i: (0, 0)),
        compiler_params=pltpu.CompilerParams(vmem_limit_bytes=56 * 2**20),
        cost_estimate=pl.CostEstimate(flops=6 * count * d_model * width, bytes_accessed=6 * d_model * width, transcendentals=count * width),
        name='gated_mlp',
    )(rows, w_gate, w_up, w_down)


def solution(mesh):
    tp_size, cp_size, dp_size = mesh.shape['tp'], mesh.shape['cp'], mesh.shape['dp']
    token_spec = P(('dp', 'cp', 'tp'), None)
    column_spec = P(None, 'tp')
    row_spec = P('tp', None)

    def layer(hidden_loc, pos_loc, cache_len, cache_k, cache_v, norm1_gain, w_query, w_key, w_value, w_out, norm2_gain, w_gate, w_up, w_down):
        _, d_model = hidden_loc.shape
        dp, tp, cp = lax.axis_index('dp'), lax.axis_index('tp'), lax.axis_index('cp')
        inv_freq = 1.0 / (ROPE_BASE ** (jnp.arange(HEAD_DIM // 2, dtype=jnp.float32) * (2.0 / HEAD_DIM)))

        def place(parts, me):
            size = len(parts)
            out = jnp.zeros((size,) + parts[0].shape, parts[0].dtype)
            for shift, part in enumerate(parts):
                out = lax.dynamic_update_index_in_dim(out, part, (me - shift) % size, 0)
            return out

        def shifted(part, axis_name, size, shift):
            return part if shift == 0 else lax.ppermute(part, axis_name, [(i, (i + shift) % size) for i in range(size)])

        def share(block):
            return place([shifted(block, 'cp', cp_size, shift) for shift in range(cp_size)], cp).reshape(-1, block.shape[-1])

        def exchange(block, split_axis):
            pieces = [lax.dynamic_index_in_dim(block, (tp + shift) % tp_size, split_axis, keepdims=False) for shift in range(tp_size)]
            return place([shifted(piece, 'tp', tp_size, shift) for shift, piece in enumerate(pieces)], tp)

        gathered = []
        for i in range(2):
            gathered.append(lax.all_gather(hidden_loc[i * RUN:(i + 1) * RUN], 'tp', axis=0, tiled=True))

        slots = cache_k.shape[0]
        cache_kv = jnp.stack([cache_k.reshape(slots, tp_size, HEAD_DIM), cache_v.reshape(slots, tp_size, HEAD_DIM)], axis=2)
        cache_kv = jnp.transpose(cache_kv.reshape(slots, tp_size, 2 * HEAD_DIM), (1, 0, 2))
        cache_kv = exchange(cache_kv, 0).reshape(tp_size * slots, 2 * HEAD_DIM)
        cache_kv = share(cache_kv)

        column_width = d_model // cp_size

        def flipped(part, flip, axis_name='cp', size=cp_size):
            return part if flip == 0 else lax.ppermute(part, axis_name, [(i, i ^ flip) for i in range(size)])

        def columns_of(array, flip):
            return lax.dynamic_slice_in_dim(array, (cp ^ flip) * column_width, column_width, 1)

        residual_columns = [flipped(columns_of(hidden_loc, flip), flip) for flip in range(cp_size)]

        def project(index, rows_in):
            rows_in = rms_norm(rows_in, norm1_gain)
            runs = cp * tp_size + jnp.arange(tp_size)
            if index == 1:
                runs = 2 * cp_size * tp_size - 1 - runs
            positions = cache_len[0] + (runs[:, None] * RUN + jnp.arange(RUN)[None, :]).reshape(-1)
            angles = positions.astype(jnp.float32)[:, None] * inv_freq[None, :]
            cos_table, sin_table = jnp.cos(angles), jnp.sin(angles)

            def rotated(weight):
                wide = jnp.dot(rows_in, weight, preferred_element_type=jnp.float32).reshape(rows_in.shape[0], -1, HEAD_DIM)
                return rotary(wide, cos_table, sin_table).reshape(rows_in.shape[0], -1)

            values = jnp.dot(rows_in, w_value, preferred_element_type=jnp.float32).astype(jnp.bfloat16)
            return rotated(w_query), jnp.concatenate([rotated(w_key), values], axis=1)

        gathered[0], cache_kv = lax.optimization_barrier((gathered[0], cache_kv))
        q_low, low_kv = project(0, gathered[0])
        low_kv = share(low_kv)
        gathered[1], q_low, low_kv, residual_columns = lax.optimization_barrier((gathered[1], q_low, low_kv, residual_columns))
        q_high, high_kv = project(1, gathered[1])
        high_kv = share(high_kv)

        w_out_local = columns_of(w_out, 0)
        half_rows = w_out.shape[0] // dp_size
        w_half = lax.dynamic_slice_in_dim(w_out_local, dp * half_rows, half_rows, 0)
        w_halves = [shifted(w_half, 'tp', tp_size, shift) for shift in range(1, tp_size)]
        low_out = attention(cache_len, q_low, cache_kv, low_kv, high_kv, True, 0, 7)

        def to_owner(out):
            blocks = out.reshape(tp_size, RUN, out.shape[1])
            return [shifted(lax.dynamic_index_in_dim(blocks, (tp + shift) % tp_size, 0, keepdims=False), 'tp', tp_size, shift) for shift in range(tp_size)]

        low_parts = to_owner(low_out)
        q_high, low_out = lax.optimization_barrier((q_high, low_out))
        w_others = [flipped(w, 1, 'dp', dp_size) for w in w_halves]
        high_a = attention(cache_len, q_high, cache_kv, low_kv, high_kv, False, 0, 4)
        high_parts_a = to_owner(high_a)

        def spread(parts):
            block = jnp.stack(parts)
            across = flipped(block, 2)
            return [block, flipped(block, 1), across, flipped(across, 1)]

        low_parts, q_high = lax.optimization_barrier((low_parts, q_high))
        low_rows = spread(low_parts)
        high_b = attention(cache_len, q_high, cache_kv, low_kv, high_kv, False, 4, 3)
        high_parts_b = to_owner(high_b)
        high_parts = [jnp.concatenate(pair, axis=1) for pair in zip(high_parts_a, high_parts_b)]
        high_rows = spread(high_parts)
        w_all = [w_out_local] + [jnp.where(dp == 0, jnp.concatenate([w, o], axis=0), jnp.concatenate([o, w], axis=0)) for w, o in zip(w_halves, w_others)]

        outs = []
        for index, spread_rows in enumerate((low_rows, high_rows)):
            if index == 1:
                spread_rows = lax.optimization_barrier((spread_rows, normed_mid))[0]
            rows = slice(index * RUN, (index + 1) * RUN)
            rows_in = jnp.concatenate(spread_rows, axis=1)
            attn_out = sum(jnp.dot(rows_in[shift], w_all[shift], preferred_element_type=jnp.float32) for shift in range(tp_size))
            mid_columns = (jnp.concatenate([r[rows] for r in residual_columns], axis=0).astype(jnp.float32) + attn_out).astype(jnp.bfloat16)
            mid = jnp.zeros((RUN, cp_size, column_width), jnp.bfloat16)
            for flip in range(cp_size):
                part = flipped(mid_columns[flip * RUN:(flip + 1) * RUN], flip)
                mid = lax.dynamic_update_slice_in_dim(mid, part[:, None, :], cp ^ flip, 1)
            mid = mid.reshape(RUN, d_model)
            normed_mid = rms_norm(mid, norm2_gain)
            group_mid = lax.all_gather(normed_mid, 'tp', axis=0, tiled=True)
            mlp_part = gated_mlp(group_mid, w_gate, w_up, w_down)
            summed = lax.psum_scatter(mlp_part, 'tp', scatter_dimension=0, tiled=True)
            outs.append((mid.astype(jnp.float32) + summed).astype(jnp.bfloat16))
        return jnp.concatenate(outs, axis=0)

    return jax.shard_map(layer, mesh=mesh, in_specs=(token_spec, P(('dp', 'cp', 'tp')), P('dp'), token_spec, token_spec, P(), column_spec, column_spec, column_spec, row_spec, P(), column_spec, column_spec, row_spec), out_specs=token_spec, check_vma=False)
```

```python
import functools
import math
import jax
import jax.numpy as jnp
from jax import lax
from jax.experimental import pallas as pl
from jax.experimental.pallas import tpu as pltpu
from jax.sharding import PartitionSpec as P

HEAD_DIM = 128
ROPE_BASE = 500000.0
NORM_EPS = 1e-5
RUN = 64
KV_BLOCK = 512
MLP_TILE = 512
LOG2E = 1.4426950408889634


def rms_norm(hidden, norm_gain):
    values = hidden.astype(jnp.float32)
    inv_rms = lax.rsqrt(jnp.mean(values * values, axis=-1, keepdims=True) + NORM_EPS)
    return (values * inv_rms * norm_gain.astype(jnp.float32)).astype(jnp.bfloat16)


def rotary(projected, cos_table, sin_table):
    half_dim = HEAD_DIM // 2
    cos_table = cos_table[:, None, :]
    sin_table = sin_table[:, None, :]
    first_half = projected[..., :half_dim]
    second_half = projected[..., half_dim:]
    rotated = jnp.concatenate([first_half * cos_table - second_half * sin_table, second_half * cos_table + first_half * sin_table], axis=-1)
    return rotated.astype(jnp.bfloat16)


def attn_kernel(is_low, clen_ref, q_ref, kc_ref, vc_ref, knl_ref, vnl_ref, knh_ref, vnh_ref, o_ref, vt_ref, m_ref, l_ref, acc_ref):
    cp = lax.axis_index('cp')
    scale = LOG2E / math.sqrt(HEAD_DIM)
    half = q_ref.shape[0]
    slots = kc_ref.shape[0]
    fresh = knl_ref.shape[0]
    cache_len = clen_ref[0]

    @pl.when(pl.program_id(0) == 0)
    def _():
        for ref, base in ((vc_ref, 0), (vnl_ref, slots), (vnh_ref, slots + fresh))[:2 if is_low else 3]:
            for j in range(ref.shape[0] // 512):
                block = ref[j * 512:(j + 1) * 512, :].astype(jnp.float32)
                vt_ref[:, base + j * 512:base + (j + 1) * 512] = block.T.astype(jnp.bfloat16)

    m_ref[...] = jnp.full_like(m_ref, -1e30)
    l_ref[...] = jnp.zeros_like(l_ref)
    acc_ref[...] = jnp.zeros_like(acc_ref)

    def update(blocks):
        scores = []
        for keys, _, mask in blocks:
            raw = lax.dot_general(keys, q_ref[...], (((1,), (1,)), ((), ())), preferred_element_type=jnp.float32)
            scores.append(raw if mask is None else jnp.where(mask, raw, -jnp.inf))
        for (_, vt_cols, _), score in zip(blocks, scores):
            m_old = m_ref[...]
            m_new = jnp.maximum(m_old, jnp.max(score, axis=0, keepdims=True))
            probs = jnp.exp2((score - m_new) * scale)
            alpha = jnp.exp2((m_old - m_new) * scale)
            l_ref[...] = alpha * l_ref[...] + jnp.sum(probs, axis=0, keepdims=True)
            acc_ref[...] = alpha * acc_ref[...] + jnp.dot(vt_ref[:, vt_cols], probs.astype(jnp.bfloat16), preferred_element_type=jnp.float32)
            m_ref[...] = m_new

    def cache_block(start):
        rows = pl.ds(pl.multiple_of(start, KV_BLOCK), KV_BLOCK)
        visible = start + lax.broadcasted_iota(jnp.int32, (KV_BLOCK, half), 0) < cache_len
        return rows, visible

    full_pairs = cache_len // (2 * KV_BLOCK)

    def cache_step(j, carry):
        first, second = (cache_block(j * 2 * KV_BLOCK + i * KV_BLOCK)[0] for i in range(2))
        update([(kc_ref[first, :], first, None), (kc_ref[second, :], second, None)])
        return carry

    lax.fori_loop(0, full_pairs, cache_step, 0)

    def tail_step(j, carry):
        rows, visible = cache_block(j * KV_BLOCK)
        update([(kc_ref[rows, :], rows, visible)])
        return carry

    lax.fori_loop(2 * full_pairs, (cache_len + KV_BLOCK - 1) // KV_BLOCK, tail_step, 0)

    def new_keys(ref, base, j, mask=None):
        start = pl.multiple_of(j * half, half)
        return ref[pl.ds(start, half), :], pl.ds(pl.multiple_of(base + start, half), half), mask

    def low_step(j, carry):
        update([new_keys(knl_ref, slots, j)])
        return carry

    key_id = lax.broadcasted_iota(jnp.int32, (half, half), 0)
    row_id = lax.broadcasted_iota(jnp.int32, (half, half), 1)
    if is_low:
        lax.fori_loop(0, cp, low_step, 0)
        update([new_keys(knl_ref, slots, cp, key_id <= row_id)])
    else:
        for j in range(0, 4, 2):
            update([new_keys(knl_ref, slots, j), new_keys(knl_ref, slots, j + 1)])

        def high_step(j, carry):
            update([new_keys(knh_ref, slots + fresh, j)])
            return carry

        lax.fori_loop(cp + 1, 4, high_step, 0)
        runs = half // RUN

        def place(i):
            return (runs - 1 - i // RUN) * RUN + i % RUN

        update([new_keys(knh_ref, slots + fresh, cp, place(key_id) <= place(row_id))])
    o_ref[...] = (acc_ref[...] / l_ref[...]).T.astype(jnp.bfloat16)


def attention(cache_len, queries, cache_kv, low_kv, high_kv, is_low, head0, heads):
    rows = queries.shape[0]
    width = heads * HEAD_DIM

    def column(array, index):
        return pl.BlockSpec((array.shape[0], HEAD_DIM), lambda g: (0, index))

    arrays = (cache_kv, low_kv, high_kv)
    return pl.pallas_call(
        functools.partial(attn_kernel, is_low),
        grid=(heads,),
        out_shape=jax.ShapeDtypeStruct((rows, width), jnp.bfloat16),
        in_specs=[pl.BlockSpec(memory_space=pltpu.SMEM), pl.BlockSpec((rows, HEAD_DIM), lambda g: (0, g + head0))]
        + [column(a, i) for a in arrays for i in range(2)],
        out_specs=pl.BlockSpec((rows, HEAD_DIM), lambda g: (0, g)),
        scratch_shapes=[pltpu.VMEM((HEAD_DIM, sum(a.shape[0] for a in arrays)), jnp.bfloat16)] + [pltpu.VMEM((1, rows), jnp.float32)] * 2 + [pltpu.VMEM((HEAD_DIM, rows), jnp.float32)],
        cost_estimate=pl.CostEstimate(flops=2 * 2 * rows * width * 4608, bytes_accessed=8 * 2**20, transcendentals=rows * heads * 4608),
        name='attend',
    )(cache_len, queries, *[a for a in arrays for _ in range(2)])


def mlp_kernel(tail, rows_ref, gate_ref, up_ref, down_ref, out_ref):
    step = pl.program_id(0)
    last = pl.num_programs(0) - 1

    @pl.when(step == 0)
    def _():
        out_ref[...] = jnp.zeros_like(out_ref)

    def tile(width):
        rows = rows_ref[...]
        gate_proj = jnp.dot(rows, gate_ref[:, :width], preferred_element_type=jnp.float32)
        up_proj = jnp.dot(rows, up_ref[:, :width], preferred_element_type=jnp.float32)
        hidden_mlp = (jax.nn.silu(gate_proj) * up_proj).astype(jnp.bfloat16)
        out_ref[...] += jnp.dot(hidden_mlp, down_ref[:width, :], preferred_element_type=jnp.float32)

    @pl.when(step < last)
    def _():
        tile(gate_ref.shape[1])

    @pl.when(step == last)
    def _():
        tile(tail)


def gated_mlp(rows, w_gate, w_up, w_down):
    count, d_model = rows.shape
    width = w_gate.shape[1]
    steps = (width + MLP_TILE - 1) // MLP_TILE
    wide = pl.BlockSpec((d_model, MLP_TILE), lambda i: (0, i))
    return pl.pallas_call(
        functools.partial(mlp_kernel, width - (steps - 1) * MLP_TILE),
        grid=(steps,),
        out_shape=jax.ShapeDtypeStruct((count, d_model), jnp.float32),
        in_specs=[pl.BlockSpec((count, d_model), lambda i: (0, 0)), wide, wide, pl.BlockSpec((MLP_TILE, d_model), lambda i: (i, 0))],
        out_specs=pl.BlockSpec((count, d_model), lambda i: (0, 0)),
        compiler_params=pltpu.CompilerParams(vmem_limit_bytes=56 * 2**20),
        cost_estimate=pl.CostEstimate(flops=6 * count * d_model * width, bytes_accessed=6 * d_model * width, transcendentals=count * width),
        name='gated_mlp',
    )(rows, w_gate, w_up, w_down)


def solution(mesh):
    tp_size, cp_size, dp_size = mesh.shape['tp'], mesh.shape['cp'], mesh.shape['dp']
    token_spec = P(('dp', 'cp', 'tp'), None)
    column_spec = P(None, 'tp')
    row_spec = P('tp', None)

    def layer(hidden_loc, pos_loc, cache_len, cache_k, cache_v, norm1_gain, w_query, w_key, w_value, w_out, norm2_gain, w_gate, w_up, w_down):
        _, d_model = hidden_loc.shape
        dp, tp, cp = lax.axis_index('dp'), lax.axis_index('tp'), lax.axis_index('cp')
        inv_freq = 1.0 / (ROPE_BASE ** (jnp.arange(HEAD_DIM // 2, dtype=jnp.float32) * (2.0 / HEAD_DIM)))

        def place(parts, me):
            size = len(parts)
            out = jnp.zeros((size,) + parts[0].shape, parts[0].dtype)
            for shift, part in enumerate(parts):
                out = lax.dynamic_update_index_in_dim(out, part, (me - shift) % size, 0)
            return out

        def shifted(part, axis_name, size, shift):
            return part if shift == 0 else lax.ppermute(part, axis_name, [(i, (i + shift) % size) for i in range(size)])

        def share(block):
            return place([shifted(block, 'cp', cp_size, shift) for shift in range(cp_size)], cp).reshape(-1, block.shape[-1])

        def exchange(block, split_axis):
            pieces = [lax.dynamic_index_in_dim(block, (tp + shift) % tp_size, split_axis, keepdims=False) for shift in range(tp_size)]
            return place([shifted(piece, 'tp', tp_size, shift) for shift, piece in enumerate(pieces)], tp)

        gathered = []
        for i in range(2):
            gathered.append(lax.all_gather(hidden_loc[i * RUN:(i + 1) * RUN], 'tp', axis=0, tiled=True))

        slots = cache_k.shape[0]
        cache_kv = jnp.stack([cache_k.reshape(slots, tp_size, HEAD_DIM), cache_v.reshape(slots, tp_size, HEAD_DIM)], axis=2)
        cache_kv = jnp.transpose(cache_kv.reshape(slots, tp_size, 2 * HEAD_DIM), (1, 0, 2))
        cache_kv = exchange(cache_kv, 0).reshape(tp_size * slots, 2 * HEAD_DIM)
        cache_kv = share(cache_kv)

        column_width = d_model // cp_size
        core, row_y = cp % 2, cp // 2

        def flipped(part, flip, axis_name='cp', size=cp_size):
            return part if flip == 0 else lax.ppermute(part, axis_name, [(i, i ^ flip) for i in range(size)])

        def columns_of(array, flip):
            return lax.dynamic_slice_in_dim(array, (cp ^ flip) * column_width, column_width, 1)

        residual_columns = [flipped(columns_of(hidden_loc, flip), flip) for flip in range(cp_size)]

        def project(index, rows_in):
            rows_in = rms_norm(rows_in, norm1_gain)
            runs = cp * tp_size + jnp.arange(tp_size)
            if index == 1:
                runs = 2 * cp_size * tp_size - 1 - runs
            positions = cache_len[0] + (runs[:, None] * RUN + jnp.arange(RUN)[None, :]).reshape(-1)
            angles = positions.astype(jnp.float32)[:, None] * inv_freq[None, :]
            cos_table, sin_table = jnp.cos(angles), jnp.sin(angles)

            def rotated(weight):
                wide = jnp.dot(rows_in, weight, preferred_element_type=jnp.float32).reshape(rows_in.shape[0], -1, HEAD_DIM)
                return rotary(wide, cos_table, sin_table).reshape(rows_in.shape[0], -1)

            values = jnp.dot(rows_in, w_value, preferred_element_type=jnp.float32).astype(jnp.bfloat16)
            return rotated(w_query), jnp.concatenate([rotated(w_key), values], axis=1)

        gathered[0], cache_kv = lax.optimization_barrier((gathered[0], cache_kv))
        q_low, low_kv = project(0, gathered[0])
        low_kv = share(low_kv)
        gathered[1], q_low, low_kv, residual_columns = lax.optimization_barrier((gathered[1], q_low, low_kv, residual_columns))
        q_high, high_kv = project(1, gathered[1])
        high_kv = share(high_kv)

        w_out_local = columns_of(w_out, 0)
        half_rows = w_out.shape[0] // dp_size
        w_half = lax.dynamic_slice_in_dim(w_out_local, dp * half_rows, half_rows, 0)
        w_halves = [shifted(w_half, 'tp', tp_size, shift) for shift in range(1, tp_size)]
        low_out = attention(cache_len, q_low, cache_kv, low_kv, high_kv, True, 0, 7)

        def to_owner(out):
            blocks = out.reshape(tp_size, RUN, out.shape[1])
            return [shifted(lax.dynamic_index_in_dim(blocks, (tp + shift) % tp_size, 0, keepdims=False), 'tp', tp_size, shift) for shift in range(tp_size)]

        low_parts = to_owner(low_out)
        q_high, low_out = lax.optimization_barrier((q_high, low_out))
        w_others = [flipped(w, 1, 'dp', dp_size) for w in w_halves]
        high_a = attention(cache_len, q_high, cache_kv, low_kv, high_kv, False, 0, 4)
        high_parts_a = to_owner(high_a)

        def spread(parts):
            block = jnp.stack(parts)
            across = flipped(block, 2)
            return [block, flipped(block, 1), across, flipped(across, 1)]

        low_parts, q_high = lax.optimization_barrier((low_parts, q_high))
        low_rows = spread(low_parts)
        high_b = attention(cache_len, q_high, cache_kv, low_kv, high_kv, False, 4, 3)
        high_parts_b = to_owner(high_b)
        high_parts = [jnp.concatenate(pair, axis=1) for pair in zip(high_parts_a, high_parts_b)]
        high_rows = spread(high_parts)
        w_all = [w_out_local] + [jnp.where(dp == 0, jnp.concatenate([w, o], axis=0), jnp.concatenate([o, w], axis=0)) for w, o in zip(w_halves, w_others)]

        outs = []
        for index, spread_rows in enumerate((low_rows, high_rows)):
            if index == 1:
                spread_rows = lax.optimization_barrier((spread_rows, normed_mid))[0]
            rows = slice(index * RUN, (index + 1) * RUN)
            rows_in = jnp.concatenate(spread_rows, axis=1)
            attn_out = sum(jnp.dot(rows_in[shift], w_all[shift], preferred_element_type=jnp.float32) for shift in range(tp_size))
            mid_columns = (jnp.concatenate([r[rows] for r in residual_columns], axis=0).astype(jnp.float32) + attn_out).astype(jnp.bfloat16)
            parts = [flipped(mid_columns[flip * RUN:(flip + 1) * RUN], flip) for flip in range(cp_size)]
            for bit, choice in ((1, core), (2, row_y)):
                parts = [jnp.where(choice == 1, parts[i ^ bit], parts[i]) for i in range(cp_size)]
            mid = jnp.concatenate(parts, axis=1)
            normed_mid = rms_norm(mid, norm2_gain)
            group_mid = lax.all_gather(normed_mid, 'tp', axis=0, tiled=True)
            mlp_part = gated_mlp(group_mid, w_gate, w_up, w_down)
            summed = lax.psum_scatter(mlp_part, 'tp', scatter_dimension=0, tiled=True)
            outs.append((mid.astype(jnp.float32) + summed).astype(jnp.bfloat16))
        return jnp.concatenate(outs, axis=0)

    return jax.shard_map(layer, mesh=mesh, in_specs=(token_spec, P(('dp', 'cp', 'tp')), P('dp'), token_spec, token_spec, P(), column_spec, column_spec, column_spec, row_spec, P(), column_spec, column_spec, row_spec), out_specs=token_spec, check_vma=False)
```
